128 devices in a mesh: row: 8 (over y, core), col: 16 (over z, x).
Axes of the slice: x: 4, y: 4, z: 4, core: 2. Of those that a mesh axis runs over, the one named last changes fastest.
Arguments:
- parent_front: float32 [8, 2048, 4, 4096], P(None, 'row', None, 'col'), may hold values from -6 to 6
- generators: bfloat16 [96, 256, 256], P('row'), may hold values from -1.5 to 1.5
- diagonal_blocks: bfloat16 [96, 256, 256], P('row'), may hold values from -6 to 6
- coupling: bfloat16 [2, 256, 256], replicated, may hold values from -0.375 to 0.375
- block_map: int32 [2, 48], replicated, may hold values from 0 to 63, as said below
- valid_rows: int32 [2, 48], replicated, may hold values from 128 to 256
Outputs:
- assembled: float32 [8, 2048, 4, 4096], P(None, 'row', None, 'col')
The draws below stay inside these ranges and needn't reach their ends.
Inputs may be any that keep to these rules, and one draw needn't show every extreme that they name: `block_map`: for each child c and each s < 4, the child blocks s * 12 to (s + 1) * 12 - 1 map in increasing order to distinct parent blocks of the range s * 16 to (s + 1) * 16 - 1, and the parent blocks s * 16 + m * 8 of that range always receive one.
All inputs are finite; a program needn't handle non-finite values.
Results may differ from the reference program's by a relative error of at most 0.0028.
Values may be sent and summed in bfloat16 or wider, within the bound.
A program may use at most 128 MiB of HBM per device.

```python
import jax
import jax.numpy as jnp
from jax import lax

BLK = 256
RANK = 256
BR_DEV = 8
PB = 64
BC_DEV = 4
WIN = 16
CG = 12
HALF = 4
CB = 48
N_ROW = 8
N_COL = 16


def draw_block_map(key, part):
    child_rows = []
    for child_index in range(2):
        pieces = []
        for group_index in range(HALF):
            window_key = jax.random.fold_in(key, 1000 * child_index + group_index + 17)
            offsets = jnp.arange(WIN, dtype=jnp.int32)
            scores = jax.random.randint(window_key, (WIN,), 0, 1 << 20, dtype=jnp.int32) * WIN + offsets
            scores = jnp.where(offsets % N_ROW == 0, jnp.int32(1 << 30), scores)
            gap_order = jnp.argsort(scores, stable=True)
            gap_slots = gap_order[:WIN - CG]
            gap_flags = jnp.zeros((WIN,), jnp.int32).at[gap_slots].set(1)
            sorted_slots = jnp.argsort(gap_flags * WIN + offsets, stable=True).astype(jnp.int32)
            chosen = sorted_slots[:CG] + WIN * group_index
            pieces.append(chosen)
        child_rows.append(jnp.concatenate(pieces))
    return jnp.stack(child_rows).astype(jnp.int32)


def place_ends(entries, own_key, low, high):
    longest = entries.shape.index(max(entries.shape))
    spots = []
    for shift in (0, 1):
        where = [jax.random.randint(jax.random.fold_in(own_key, axis), (), 0, length) for axis, length in enumerate(entries.shape)]
        where[longest] = (where[longest] + shift) % entries.shape[longest]
        spots.append(tuple(where))
    return entries.at[spots[0]].set(low).at[spots[1]].set(high)


def shard_levels(own_key, extent, cuts, smallest, largest):
    def one(dim, blocks):
        heights = jax.random.uniform(jax.random.fold_in(jax.random.fold_in(own_key, 6), dim), (blocks,), jnp.float32, smallest / len(cuts), largest / len(cuts))
        return jnp.repeat(jnp.exp(heights), extent[dim] // blocks).reshape((-1,) + (1,) * (len(extent) - dim - 1))

    loudness = one(*cuts[0])
    for cut in cuts[1:]:
        loudness = loudness * one(*cut)
    return loudness


def bell_draw(stream_key, dims, scale, reach, cuts=(), held_as=jnp.bfloat16):
    entries = jax.random.normal(stream_key, dims, jnp.float32) * scale
    if len(cuts) > 0:
        entries = shard_levels(stream_key, dims, cuts, -0.22, 0.18) * entries
    return jnp.clip(entries, min=-reach, max=reach).astype(held_as)


def setup_inputs(seed: int = 0) -> dict:
    arg_keys = jax.random.split(jax.random.key(seed), 7)
    parent_front = bell_draw(arg_keys[0], (BR_DEV, N_ROW * BLK, BC_DEV, N_COL * BLK), 1.0, 6.0, ((1, 8), (3, 16)), jnp.float32)
    generators = bell_draw(arg_keys[1], (2 * CB, BLK, RANK), 0.25, 1.5, ((0, 8),))
    diagonal_blocks = bell_draw(arg_keys[2], (2 * CB, BLK, BLK), 1.0, 6.0, ((0, 8),))
    coupling = bell_draw(arg_keys[3], (2, RANK, RANK), RANK ** -0.5, 0.375)
    block_map = draw_block_map(jax.random.fold_in(arg_keys[6], 71), 0)
    valid_rows = place_ends(jax.random.randint(arg_keys[5], (2, CB), BLK // 2, BLK + 1), jax.random.fold_in(arg_keys[5], 1), BLK // 2, BLK).astype(jnp.int32)
    return dict(parent_front=parent_front, generators=generators, diagonal_blocks=diagonal_blocks, coupling=coupling, block_map=block_map, valid_rows=valid_rows)


def child_select(stacked, child_index):
    grouped = stacked.reshape((HALF, 2, CG) + stacked.shape[1:])
    return grouped[:, child_index].reshape((CB,) + stacked.shape[1:])


def child_parts(gen_blocks, diag_rows, coupling_one, map_row, count_row):
    row_offsets = jnp.arange(BLK, dtype=jnp.int32)
    kept_mask = (row_offsets[None, :] < count_row[:, None]).astype(jnp.float32)
    masked = gen_blocks.astype(jnp.float32) * kept_mask[:, :, None]
    projected = jnp.einsum("ixq,qr->ixr", masked, coupling_one.astype(jnp.float32)).astype(jnp.bfloat16)
    diag_kept = diag_rows.astype(jnp.float32) * kept_mask[:, :, None] * kept_mask[:, None, :]
    placing = (map_row[None, :] == jnp.arange(PB, dtype=jnp.int32)[:, None]).astype(jnp.float32)
    placed_gen = jnp.einsum("pi,ixq->pxq", placing, masked)
    placed_proj = jnp.einsum("pi,ixq->pxq", placing, projected.astype(jnp.float32))
    placed_diag = jnp.einsum("pi,ixz->pxz", placing, diag_kept)
    return placed_gen, placed_proj, placed_diag


def reference(parent_front, generators, diagonal_blocks, coupling, block_map, valid_rows):
    front_blocks = parent_front.reshape(PB, BLK, PB, BLK)
    child_data = [child_parts(child_select(generators, child_index),
                              child_select(diagonal_blocks, child_index),
                              coupling[child_index], block_map[child_index], valid_rows[child_index])
                  for child_index in range(2)]
    placed_gen = jnp.stack([child_data[0][0], child_data[1][0]], axis=1)
    placed_proj = jnp.stack([child_data[0][1], child_data[1][1]])
    placed_diag = jnp.stack([child_data[0][2], child_data[1][2]], axis=1)
    block_ids = jnp.arange(PB, dtype=jnp.int32)

    def one_row(row_items):
        front_row, gen_row, diag_row, row_id = row_items
        on_diag = (block_ids == row_id).astype(jnp.float32)
        running = front_row
        for child_index in range(2):
            child_tile = jnp.einsum("xq,jzq->xjz", gen_row[child_index], placed_proj[child_index])
            child_tile = child_tile + diag_row[child_index][:, None, :] * on_diag[None, :, None]
            rounded = lax.optimization_barrier(child_tile.astype(jnp.bfloat16))
            running = running + rounded.astype(jnp.float32)
        return running

    rows_out = lax.map(one_row, (front_blocks, placed_gen, placed_diag, block_ids))
    return rows_out.reshape(BR_DEV, N_ROW * BLK, BC_DEV, N_COL * BLK)
```

```python
import jax
import jax.numpy as jnp
from jax import lax
from jax.experimental import pallas as pl
from jax.experimental.pallas import tpu as pltpu
from jax.sharding import PartitionSpec as P

MESH = pl.DeviceIdType.MESH
CHIPS = 4
CORES = 2
SIDE = 4
GROUP = 12
WINDOW = 16
STRIPS = 16
BLK = 256
STRIP = BLK // STRIPS
UNITS = 2 * CHIPS
LANES = 128
HALF = BLK // 2


def semaphore_table():
    names = []
    for h in range(2):
        names += [("A1", h, d) for d in (1, -1)]
        names += [("A2", h, d) for d in (1, -1)]
        names += [("B1", h, i, d) for i in ("own", 1, -1, 2, -2) for d in (1, -1)]
        names += [("B2", h, i, 1) for i in ("own", 1, -1, 2)]
        names += [("B2", h, i, -1) for i in ("own", 1, -1, -2)]
    names += [("S", i) for i in range(6)]
    names += [("PR",)]
    for part in range(2):
        names += [("CP", part)]
        for d in (1, -1):
            names += [("C", part, d), ("CF", part, d), ("CN", part, d), ("CQ", part, d)]
    return {name: i for i, name in enumerate(names)}


SEMS = semaphore_table()


def gather_kernel(bmap, gen, diag, parent, g, cd, front, gp, gv, dv, sb, pb, lsem, ssem, rsem):
    r = lax.axis_index("row")
    t = lax.axis_index("col")
    y, c = r // CORES, r % CORES
    z, x = t // SIDE, t % SIDE
    partner = (y * CORES + 1 - c, t)

    def wrap(v):
        return (v + 8) % 4

    def ydev(step, core):
        return (wrap(y + step) * CORES + core, t)

    load_strip = pltpu.make_async_copy(gen.at[:, pl.ds(t * STRIP, STRIP), :], gp, lsem.at[0])
    load_gen = pltpu.make_async_copy(gen, gv, lsem.at[1])
    load_diag = pltpu.make_async_copy(diag, dv, lsem.at[2])
    load_front = pltpu.make_async_copy(parent, front, lsem.at[3])
    load_strip.start()
    load_gen.start()
    load_diag.start()
    load_front.start()

    barrier = pltpu.get_barrier_semaphore()
    peers = [ydev(s, k) for s in (1, 2, 3) for k in range(CORES)] + [partner]
    for s in (1, -1):
        peers += [(r, z * SIDE + wrap(x + s)), (r, wrap(z + s) * SIDE + x)]
    for peer in peers:
        pl.semaphore_signal(barrier, inc=1, device_id=peer, device_id_type=MESH)

    entries = [bmap[c, y * GROUP + i] for i in range(GROUP)]

    def source(slot):
        at = y * WINDOW + slot
        before = jnp.int32(0)
        for e in entries:
            before = before + jnp.where(e < at, 1, 0).astype(jnp.int32)
        return jnp.minimum(before, GROUP - 1)

    load_strip.wait()
    for d in (1, 2, 3):
        for k in range(CORES):
            for m in range(2):
                slot = m * 8 + CORES * wrap(y - d) + k
                sb[(d - 1) * CORES + k, m] = gp[source(slot)]
    load_gen.wait()
    cd[c, y, 0] = gv[source(t)]
    for m in range(2):
        g[c, :, m] = gv[source(m * 8 + r)].reshape(STRIPS, STRIP, BLK)
        pb[:, m] = gv[source(m * 8 + y * CORES + 1 - c)].reshape(STRIPS, STRIP, BLK)
    load_diag.wait()
    cd[c, y, 1] = dv[source(t)]

    pl.semaphore_wait(barrier, len(peers))

    sent = []

    def send(name, src, dst, to, recv=None):
        k = SEMS[name]
        copy = pltpu.make_async_remote_copy(
            src_ref=src, dst_ref=dst, send_sem=ssem.at[k], recv_sem=rsem.at[k if recv is None else recv],
            device_id=to, device_id_type=MESH,
        )
        copy.start()
        sent.append(copy)

    def arrived(name, ref):
        k = SEMS[name]
        pltpu.make_async_remote_copy(
            src_ref=ref, dst_ref=ref, send_sem=ssem.at[k], recv_sem=rsem.at[k],
            device_id=partner, device_id_type=MESH,
        ).wait_recv()

    for d in (2, 1, 3):
        for k in range(CORES):
            i = (d - 1) * CORES + k
            send(("S", i), sb.at[i], g.at[c, t, pl.ds(2 * d, 2)], ydev(-d, k), SEMS[("S", 0)] + (d - 1) * CORES + c)
    for part in range(2):
        for d in (1, -1):
            send(("C", part, d), cd.at[c, y, part], cd.at[c, y, part], ydev(d, c))
    send(("PR",), pb, g.at[c, :, pl.ds(0, 2)], partner)
    for part in range(2):
        send(("CP", part), cd.at[c, y, part], cd.at[c, y, part], partner)

    pos = [(x, z), (z, x)]

    def dev(h, dp, dq):
        p, q = wrap(pos[h][0] + dp), wrap(pos[h][1] + dq)
        return (r, q * SIDE + p) if h == 0 else (r, p * SIDE + q)

    def piece(h, dp, dq, part=None):
        at = dev(h, dp, dq)[1]
        if part is None:
            return g.at[h, at, pl.ds(2, 6)]
        return g.at[h, at, pl.ds(2 + 3 * part, 3)]

    def item_ref(h, item, dq):
        if item == "own":
            return piece(h, 0, dq)
        if item in (1, -1):
            return piece(h, item, dq)
        return piece(h, 2, dq, 0 if item == 2 else 1)

    def half_ref(h, item, dq, part):
        if item == "own":
            return piece(h, 0, dq, part)
        if item in (1, -1):
            return piece(h, item, dq, part)
        return piece(h, 2, dq, part)

    def first_q(h, item):
        for d in (1, -1):
            ref = item_ref(h, item, 0)
            send(("B1", h, item, d), ref, ref, dev(h, 0, d))

    def second_q(h, item):
        for d in (1, -1):
            part = 0 if d == 1 else 1
            if item not in (2, -2):
                arrived(("B1", h, item, d), item_ref(h, item, -d))
                ref = half_ref(h, item, -d, part)
                send(("B2", h, item, d), ref, ref, dev(h, 0, d))

    def second_q_far(h):
        for d in (1, -1):
            for item in (2, -2):
                arrived(("B1", h, item, d), item_ref(h, item, -d))
        for d in (1, -1):
            item = 2 * d
            ref = item_ref(h, item, -d)
            send(("B2", h, item, d), ref, ref, dev(h, 0, d))

    for h in range(2):
        for d in (1, 2, 3):
            arrived(("S", (d - 1) * CORES + h), g.at[h, t, pl.ds(2 * d, 2)])
    for h in range(2):
        for d in (1, -1):
            ref = piece(h, 0, 0)
            send(("A1", h, d), ref, ref, dev(h, d, 0))
    for h in range(2):
        first_q(h, "own")

    def near(part):
        for d in (1, -1):
            ref = cd.at[c, wrap(y - d), part]
            arrived(("C", part, d), ref)
            half = cd.at[c, wrap(y - d), part, pl.ds(0 if d == 1 else HALF, HALF)]
            send(("CF", part, d), half, half, ydev(d, c))
            send(("CN", part, d), ref, ref, partner)

    def far(part):
        for d in (1, -1):
            half = cd.at[c, wrap(y + 2), part, pl.ds(0 if d == 1 else HALF, HALF)]
            arrived(("CF", part, d), half)
            send(("CQ", part, d), half, half, partner)

    near(0)
    for h in range(2):
        for d in (1, -1):
            arrived(("A1", h, d), piece(h, -d, 0))
            ref = piece(h, -d, 0, 0 if d == 1 else 1)
            send(("A2", h, d), ref, ref, dev(h, d, 0))
        for d in (1, -1):
            first_q(h, -d)
    for h in range(2):
        second_q(h, "own")
    for h in range(2):
        for d in (1, -1):
            arrived(("A2", h, d), piece(h, 2, 0, 0 if d == 1 else 1))
            first_q(h, 2 * d)
    near(1)
    far(0)
    for h in range(2):
        for d in (1, -1):
            second_q(h, d)
    for h in range(2):
        second_q_far(h)
    far(1)

    for h in range(2):
        for d in (1, -1):
            part = 0 if d == 1 else 1
            for item in ("own", 1, -1, 2 * d):
                arrived(("B2", h, item, d), half_ref(h, item, 2, part))
    other = 1 - c
    arrived(("PR",), g.at[other, :, pl.ds(0, 2)])
    for part in range(2):
        arrived(("CP", part), cd.at[other, y, part])
        for d in (1, -1):
            arrived(("CN", part, d), cd.at[other, wrap(y - d), part])
            arrived(("CQ", part, d), cd.at[other, wrap(y + 2), part, pl.ds(0 if d == 1 else HALF, HALF)])
    load_front.wait()
    for copy in sent:
        copy.wait_send()


def tile_kernel(bmap, vrows, g, cd, coup, front, out, pscr, ascr):
    r = lax.axis_index("row")
    t = lax.axis_index("col")
    y = r // CORES
    a = pl.program_id(0)

    def kept(child, group, parent_block):
        total = jnp.int32(0)
        for i in range(GROUP):
            at = group * GROUP + i
            total = total + jnp.where(bmap[child, at] == parent_block, vrows[child, at], 0)
        return total

    rows = lax.broadcasted_iota(jnp.int32, (BLK, BLK), 0)

    @pl.when(a == 0)
    def _():
        for s in range(CHIPS):
            for child in range(2):
                count = kept(child, s, s * WINDOW + t)
                col = jnp.where(rows < count, cd[child, s, 0], jnp.zeros((BLK, BLK), jnp.bfloat16))
                proj = jnp.dot(col, coup[child], preferred_element_type=jnp.float32)
                pscr[s, :, child * BLK:(child + 1) * BLK] = proj.astype(jnp.bfloat16)

    s, m = a // 2, a % 2
    away = (s - y + CHIPS) % CHIPS
    for child in range(2):
        count = kept(child, s, a * 8 + r)
        block = g[child, :, 2 * away + m].reshape(BLK, BLK)
        ascr[:, child * BLK:(child + 1) * BLK] = jnp.where(rows < count, block, jnp.zeros((BLK, BLK), jnp.bfloat16))
    dst = out.at[0]
    src = front.at[a]
    for b in range(CHIPS):
        tile = lax.dot_general(
            ascr[...], pscr[b], (((1,), (1,)), ((), ())), preferred_element_type=jnp.float32
        )
        for side in range(2):
            at = pl.ds(side * CHIPS + b, BLK, stride=8)
            dst[at, :] = src[at, :] + tile[:, side * LANES:(side + 1) * LANES]

    @pl.when(jnp.logical_and(r == t % 8, m == t // 8))
    def _():
        cols = lax.broadcasted_iota(jnp.int32, (BLK, LANES), 1)
        down = lax.broadcasted_iota(jnp.int32, (BLK, LANES), 0)
        for side in range(2):
            at = pl.ds(side * CHIPS + s, BLK, stride=8)
            total = dst[at, :]
            for child in range(2):
                count = kept(child, s, a * 8 + r)
                inside = jnp.logical_and(down < count, cols + side * LANES < count)
                part = cd[child, s, 1, :, side * LANES:(side + 1) * LANES].astype(jnp.float32)
                total = total + jnp.where(inside, part, 0.0)
            dst[at, :] = total


def shards(parent_front, generators, diagonal_blocks, coupling, block_map, valid_rows):
    flat = parent_front.reshape(8, BLK, CHIPS, 2, LANES).transpose(0, 1, 3, 2, 4).reshape(8, BLK * 8, LANES)
    any_spec = pl.BlockSpec(memory_space=pl.ANY)
    vmem = pl.BlockSpec(memory_space=pltpu.VMEM)
    smem = pl.BlockSpec(memory_space=pltpu.SMEM)
    bf16 = jnp.bfloat16
    g, cd, front = pl.pallas_call(
        gather_kernel,
        name="gather",
        in_specs=[smem, any_spec, any_spec, any_spec],
        out_specs=[vmem, vmem, vmem],
        out_shape=[
            pltpu.VMEM((2, STRIPS, UNITS, STRIP, BLK), bf16),
            pltpu.VMEM((2, CHIPS, 2, BLK, BLK), bf16),
            pltpu.VMEM((8, BLK * 8, LANES), jnp.float32),
        ],
        scratch_shapes=[
            pltpu.VMEM((GROUP, STRIP, BLK), bf16),
            pltpu.VMEM((GROUP, BLK, BLK), bf16),
            pltpu.VMEM((GROUP, BLK, BLK), bf16),
            pltpu.VMEM((6, 2, STRIP, BLK), bf16),
            pltpu.VMEM((STRIPS, 2, STRIP, BLK), bf16),
            pltpu.SemaphoreType.DMA((4,)),
            pltpu.SemaphoreType.DMA((len(SEMS),)),
            pltpu.SemaphoreType.DMA((len(SEMS),)),
        ],
        compiler_params=pltpu.CompilerParams(
            collective_id=0, has_side_effects=True, vmem_limit_bytes=48 << 20
        ),
    )(block_map, generators, diagonal_blocks, flat)
    out = pl.pallas_call(
        tile_kernel,
        name="tiles",
        grid=(8,),
        in_specs=[smem, smem, vmem, vmem, vmem, vmem],
        out_specs=pl.BlockSpec((1, BLK * 8, LANES), lambda a: (a, 0, 0)),
        out_shape=jax.ShapeDtypeStruct((8, BLK * 8, LANES), jnp.float32),
        scratch_shapes=[
            pltpu.VMEM((CHIPS, BLK, 2 * BLK), bf16),
            pltpu.VMEM((BLK, 2 * BLK), bf16),
        ],
        compiler_params=pltpu.CompilerParams(vmem_limit_bytes=40 << 20),
    )(block_map, valid_rows, g, cd, coupling, front)
    return out.reshape(8, BLK, 2, CHIPS, LANES).transpose(0, 1, 3, 2, 4).reshape(8, BLK, CHIPS, BLK)


def solution(mesh):
    in_specs = (
        P(None, "row", None, "col"),
        P("row", None, None),
        P("row", None, None),
        P(),
        P(),
        P(),
    )
    out_specs = P(None, "row", None, "col")
    return jax.shard_map(shards, mesh=mesh, in_specs=in_specs, out_specs=out_specs, check_vma=False)
```

```python
import jax
import jax.numpy as jnp
from jax import lax
from jax.experimental import pallas as pl
from jax.experimental.pallas import tpu as pltpu
from jax.sharding import PartitionSpec as P

MESH = pl.DeviceIdType.MESH
CHIPS = 4
CORES = 2
SIDE = 4
GROUP = 12
WINDOW = 16
STRIPS = 16
BLK = 256
STRIP = BLK // STRIPS
UNITS = 2 * CHIPS
LANES = 128
HALF = BLK // 2


def semaphore_table():
    names = []
    for m in range(2):
        names += [("A1", m, d) for d in (1, -1)]
        names += [("A2", m, d) for d in (1, -1)]
        names += [("B1", m, i, d) for i in ("own", 1, -1, 2, -2) for d in (1, -1)]
        names += [("B2", m, i, 1) for i in ("own", 1, -1, 2)]
        names += [("B2", m, i, -1) for i in ("own", 1, -1, -2)]
        names += [("S", m, i) for i in range(6)]
        names += [("PR", m)]
    for part in range(2):
        names += [("CP", part)]
        for d in (1, -1):
            names += [("C", part, d, k) for k in range(2)]
            names += [("CF", part, d), ("CN", part, d), ("CQ", part, d)]
    return {name: i for i, name in enumerate(names)}


SEMS = semaphore_table()


def gather_kernel(
    bmap, vrows, gen, diag, coup, parent, front, g, cd, gp, gv, dv, cw, sb, pb, pt, ascr, lsem, ssem, rsem
):
    r = lax.axis_index("row")
    t = lax.axis_index("col")
    y, c = r // CORES, r % CORES
    z, x = t // SIDE, t % SIDE
    other = 1 - c
    partner = (y * CORES + other, t)
    pos = [(x, z), (z, x)]

    def wrap(v):
        return (v + 8) % 4

    def ydev(step, core):
        return (wrap(y + step) * CORES + core, t)

    def dev(m, dp, dq):
        p, q = wrap(pos[m][0] + dp), wrap(pos[m][1] + dq)
        return (r, q * SIDE + p) if m == 0 else (r, p * SIDE + q)

    def strip(m, dp, dq):
        return wrap(pos[m][1] + dq) * SIDE + wrap(pos[m][0] + dp)

    load_strips = [
        pltpu.make_async_copy(gen.at[:, pl.ds(strip(m, 0, 0) * STRIP, STRIP), :], gp.at[m], lsem.at[m])
        for m in range(2)
    ]
    load_gen = pltpu.make_async_copy(gen, gv, lsem.at[2])
    load_diag = pltpu.make_async_copy(diag, dv, lsem.at[3])
    load_coup = pltpu.make_async_copy(coup, cw, lsem.at[4])
    load_front = pltpu.make_async_copy(parent, front, lsem.at[5])
    for load in load_strips:
        load.start()

    barrier = pltpu.get_barrier_semaphore()
    peers = [ydev(s, k) for s in (1, 2, 3) for k in range(CORES)] + [partner]
    peers += [dev(0, s, 0) for s in (1, -1)] + [dev(1, s, 0) for s in (1, -1)]
    for peer in peers:
        pl.semaphore_signal(barrier, inc=1, device_id=peer, device_id_type=MESH)
    load_gen.start()
    load_diag.start()
    load_coup.start()

    entries = [bmap[c, y * GROUP + i] for i in range(GROUP)]

    def source(slot):
        at = y * WINDOW + slot
        before = jnp.int32(0)
        for e in entries:
            before = before + jnp.where(e < at, 1, 0).astype(jnp.int32)
        return jnp.minimum(before, GROUP - 1)

    def kept(child, group, parent_block):
        total = jnp.int32(0)
        for i in range(GROUP):
            at = group * GROUP + i
            total = total + jnp.where(bmap[child, at] == parent_block, vrows[child, at], 0)
        return total

    for load in load_strips:
        load.wait()
    for m in range(2):
        for d in (2, 1, 3):
            for k in range(CORES):
                sb[m, (d - 1) * CORES + k] = gp[m, source(m * 8 + CORES * wrap(y - d) + k)]

    pl.semaphore_wait(barrier, len(peers))

    sent = []

    def send(name, src, dst, to, recv=None):
        k = SEMS[name]
        copy = pltpu.make_async_remote_copy(
            src_ref=src, dst_ref=dst, send_sem=ssem.at[k], recv_sem=rsem.at[k if recv is None else recv],
            device_id=to, device_id_type=MESH,
        )
        copy.start()
        sent.append(copy)

    def arrived(name, ref):
        k = SEMS[name]
        pltpu.make_async_remote_copy(
            src_ref=ref, dst_ref=ref, send_sem=ssem.at[k], recv_sem=rsem.at[k],
            device_id=partner, device_id_type=MESH,
        ).wait_recv()

    for d in (2, 1, 3):
        for m in range(2):
            for k in range(CORES):
                i = (d - 1) * CORES + k
                send(
                    ("S", m, i), sb.at[m, i], g.at[m, strip(m, 0, 0), 2 * d + c],
                    ydev(-d, k), SEMS[("S", m, 0)] + (d - 1) * CORES + c,
                )
    load_gen.wait()
    cd[c, y, 0] = gv[source(t)]
    for m in range(2):
        pb[m] = gv[source(m * 8 + y * CORES + other)].reshape(STRIPS, STRIP, BLK)

    def rows_of(k):
        return pl.ds(k * HALF, HALF)

    def onward(d):
        return 0 if d == 1 else 1

    def send_own(part, lead):
        for d in (1, -1):
            k = onward(d) if lead else 1 - onward(d)
            ref = cd.at[c, y, part, rows_of(k)]
            send(("C", part, d, k), ref, ref, ydev(d, c))

    send_own(0, True)
    send_own(0, False)
    send(("CP", 0), cd.at[c, y, 0], cd.at[c, y, 0], partner)
    for m in range(2):
        send(("PR", m), pb.at[m], g.at[m, :, c], partner)
        g[m, :, c] = gv[source(m * 8 + r)].reshape(STRIPS, STRIP, BLK)
    load_diag.wait()
    cd[c, y, 1] = dv[source(t)]
    load_front.start()
    send_own(1, True)

    def piece(m, dp, dq, part=None):
        at = strip(m, dp, dq)
        if part is None:
            return g.at[m, at, pl.ds(2, 6)]
        return g.at[m, at, pl.ds(2 + 3 * part, 3)]

    def item_ref(m, item, dq):
        if item == "own":
            return piece(m, 0, dq)
        if item in (1, -1):
            return piece(m, item, dq)
        return piece(m, 2, dq, 0 if item == 2 else 1)

    def half_ref(m, item, dq, part):
        if item == "own":
            return piece(m, 0, dq, part)
        if item in (1, -1):
            return piece(m, item, dq, part)
        return piece(m, 2, dq, part)

    def first_q(m, item):
        for d in (1, -1):
            ref = item_ref(m, item, 0)
            send(("B1", m, item, d), ref, ref, dev(m, 0, d))

    def second_q(m, item):
        for d in (1, -1):
            arrived(("B1", m, item, d), item_ref(m, item, -d))
            ref = half_ref(m, item, -d, onward(d))
            send(("B2", m, item, d), ref, ref, dev(m, 0, d))

    def second_q_far(m):
        for d in (1, -1):
            for item in (2, -2):
                arrived(("B1", m, item, d), item_ref(m, item, -d))
        for d in (1, -1):
            item = 2 * d
            ref = item_ref(m, item, -d)
            send(("B2", m, item, d), ref, ref, dev(m, 0, d))

    def relay(part):
        for d in (1, -1):
            k = onward(d)
            half = cd.at[c, wrap(y - d), part, rows_of(k)]
            arrived(("C", part, d, k), half)
            send(("CF", part, d), half, half, ydev(d, c))

    def near(part):
        for d in (1, -1):
            k = 1 - onward(d)
            arrived(("C", part, d, k), cd.at[c, wrap(y - d), part, rows_of(k)])
            ref = cd.at[c, wrap(y - d), part]
            send(("CN", part, d), ref, ref, partner)

    def far(part):
        for d in (1, -1):
            half = cd.at[c, wrap(y + 2), part, rows_of(onward(d))]
            arrived(("CF", part, d), half)
            send(("CQ", part, d), half, half, partner)

    def partner_blocks(part):
        arrived(("CP", part), cd.at[other, y, part])
        for d in (1, -1):
            arrived(("CN", part, d), cd.at[other, wrap(y - d), part])
            arrived(("CQ", part, d), cd.at[other, wrap(y + 2), part, rows_of(onward(d))])

    zero = jnp.zeros((), jnp.bfloat16)
    down = lax.broadcasted_iota(jnp.int32, (BLK, BLK), 0)

    def project(s, _):
        for child in range(2):
            count = kept(child, s, s * WINDOW + t)
            col = jnp.where(down < count, cd[child, s, 0], zero)
            proj = lax.dot_general(
                cw[child], col, (((0,), (1,)), ((), ())), preferred_element_type=jnp.float32
            )
            pt[s, child * BLK:(child + 1) * BLK, :] = proj.astype(jnp.bfloat16)
        return 0

    def add_tiles(m, groups, first, rows, unroll):
        for n, d in enumerate(groups):
            s = wrap(y + d)
            for child in range(2):
                count = kept(child, s, (2 * s + m) * 8 + r)
                block = g[m, pl.ds(first, rows // STRIP), 2 * d + child].reshape(rows, BLK)
                inside = down[:rows] + first * STRIP < count
                ascr[n * rows:(n + 1) * rows, child * BLK:(child + 1) * BLK] = jnp.where(inside, block, zero)

        def column(b):
            tile = jnp.dot(
                ascr[:len(groups) * rows, :], pt[b], preferred_element_type=jnp.float32
            )
            for n, d in enumerate(groups):
                dst = front.at[2 * wrap(y + d) + m]
                for side in range(2):
                    at = pl.ds(first * STRIP * 8 + side * CHIPS + b, rows, stride=8)
                    dst[at, :] = dst[at, :] + tile[n * rows:(n + 1) * rows, side * LANES:(side + 1) * LANES]

        @pl.loop(0, CHIPS // unroll)
        def _(i):
            for k in range(unroll):
                column(i * unroll + k)

    def quarter(m, dq):
        line = z * (1 - m) + x * m
        add_tiles(m, (1, 2, 3), SIDE * wrap(line + dq), SIDE * STRIP, 2)

    def add_diagonals():
        cols = lax.broadcasted_iota(jnp.int32, (BLK, LANES), 1)
        for b in range(CHIPS):
            dst = front.at[2 * b + t // 8]
            for side in range(2):
                at = pl.ds(side * CHIPS + b, BLK, stride=8)
                total = dst[at, :]
                for child in range(2):
                    count = kept(child, b, b * WINDOW + t)
                    inside = jnp.logical_and(down[:, :LANES] < count, cols + side * LANES < count)
                    block = cd[child, b, 1, :, side * LANES:(side + 1) * LANES].astype(jnp.float32)
                    total = total + jnp.where(inside, block, 0.0)
                dst[at, :] = total

    for m in range(2):
        for d in (1, 2, 3):
            for k in range(CORES):
                arrived(("S", m, (d - 1) * CORES + k), g.at[m, strip(m, 0, 0), 2 * d + k])
    for m in range(2):
        for d in (1, -1):
            ref = piece(m, 0, 0)
            send(("A1", m, d), ref, ref, dev(m, d, 0))
    for m in range(2):
        first_q(m, "own")
    send(("CP", 1), cd.at[c, y, 1], cd.at[c, y, 1], partner)
    relay(0)
    send_own(1, False)
    near(0)
    for m in range(2):
        for d in (1, -1):
            arrived(("A1", m, d), piece(m, -d, 0))
            ref = piece(m, -d, 0, onward(d))
            send(("A2", m, d), ref, ref, dev(m, d, 0))
        for d in (1, -1):
            first_q(m, -d)
    for m in range(2):
        second_q(m, "own")
    relay(1)
    for m in range(2):
        for d in (1, -1):
            arrived(("A2", m, d), piece(m, 2, 0, onward(d)))
            first_q(m, 2 * d)
    far(0)
    load_front.wait()
    load_coup.wait()
    for m in range(2):
        for d in (1, -1):
            second_q(m, d)
    near(1)
    partner_blocks(0)
    lax.fori_loop(0, CHIPS, project, 0)
    for m in range(2):
        second_q_far(m)
    far(1)
    for m in range(2):
        arrived(("PR", m), g.at[m, :, other])

    @pl.loop(0, 2)
    def _(m):
        add_tiles(m, (0,), 0, BLK, 1)

    @pl.loop(0, 6)
    def _(i):
        quarter(i // 3, i % 3 - 1)

    partner_blocks(1)

    @pl.when(r == t % 8)
    def _():
        add_diagonals()

    for m in range(2):
        for d in (1, -1):
            for item in ("own", 1, -1, 2 * d):
                arrived(("B2", m, item, d), half_ref(m, item, 2, onward(d)))

    @pl.loop(0, 2)
    def _(m):
        quarter(m, 2)

    for copy in sent:
        copy.wait_send()


def write_kernel(front, out, sems):
    copies = [pltpu.make_async_copy(front.at[a], out.at[a], sems.at[a]) for a in range(8)]
    for copy in copies:
        copy.start()
    for copy in copies:
        copy.wait()


def shards(parent_front, generators, diagonal_blocks, coupling, block_map, valid_rows):
    flat = parent_front.reshape(8, BLK, CHIPS, 2, LANES).transpose(0, 1, 3, 2, 4).reshape(8, BLK * 8, LANES)
    any_spec = pl.BlockSpec(memory_space=pl.ANY)
    vmem = pl.BlockSpec(memory_space=pltpu.VMEM)
    smem = pl.BlockSpec(memory_space=pltpu.SMEM)
    bf16 = jnp.bfloat16
    front = pl.pallas_call(
        gather_kernel,
        name="gather",
        in_specs=[smem, smem, any_spec, any_spec, any_spec, any_spec],
        out_specs=vmem,
        out_shape=pltpu.VMEM((8, BLK * 8, LANES), jnp.float32),
        scratch_shapes=[
            pltpu.VMEM((2, STRIPS, UNITS, STRIP, BLK), bf16),
            pltpu.VMEM((2, CHIPS, 2, BLK, BLK), bf16),
            pltpu.VMEM((2, GROUP, STRIP, BLK), bf16),
            pltpu.VMEM((GROUP, BLK, BLK), bf16),
            pltpu.VMEM((GROUP, BLK, BLK), bf16),
            pltpu.VMEM((2, BLK, BLK), bf16),
            pltpu.VMEM((2, 6, STRIP, BLK), bf16),
            pltpu.VMEM((2, STRIPS, STRIP, BLK), bf16),
            pltpu.VMEM((CHIPS, 2 * BLK, BLK), bf16),
            pltpu.VMEM((BLK, 2 * BLK), bf16),
            pltpu.SemaphoreType.DMA((6,)),
            pltpu.SemaphoreType.DMA((len(SEMS),)),
            pltpu.SemaphoreType.DMA((len(SEMS),)),
        ],
        compiler_params=pltpu.CompilerParams(
            collective_id=0, has_side_effects=True, vmem_limit_bytes=52 << 20
        ),
    )(block_map, valid_rows, generators, diagonal_blocks, coupling, flat)
    out = pl.pallas_call(
        write_kernel,
        name="write",
        in_specs=[vmem],
        out_specs=any_spec,
        out_shape=jax.ShapeDtypeStruct((8, BLK * 8, LANES), jnp.float32),
        scratch_shapes=[pltpu.SemaphoreType.DMA((8,))],
        compiler_params=pltpu.CompilerParams(vmem_limit_bytes=1 << 20),
    )(front)
    return out.reshape(8, BLK, 2, CHIPS, LANES).transpose(0, 1, 3, 2, 4).reshape(8, BLK, CHIPS, BLK)


def solution(mesh):
    in_specs = (
        P(None, "row", None, "col"),
        P("row", None, None),
        P("row", None, None),
        P(),
        P(),
        P(),
    )
    out_specs = P(None, "row", None, "col")
    return jax.shard_map(shards, mesh=mesh, in_specs=in_specs, out_specs=out_specs, check_vma=False)
```

```python
import jax
import jax.numpy as jnp
from jax import lax
from jax.experimental import pallas as pl
from jax.experimental.pallas import tpu as pltpu
from jax.sharding import PartitionSpec as P

MESH = pl.DeviceIdType.MESH
CHIPS = 4
CORES = 2
SIDE = 4
GROUP = 12
WINDOW = 16
STRIPS = 16
BLK = 256
STRIP = BLK // STRIPS
LANES = 128
HALF = BLK // 2
BANDS = 8


def semaphore_table():
    names = []
    for m in range(2):
        names += [("A1", m, d) for d in (1, -1)]
        names += [("A2", m, d) for d in (1, -1)]
        names += [("B1", m, i, d) for i in ("own", 1, -1, 2, -2) for d in (1, -1)]
        names += [("B2", m, i, 1) for i in ("own", 1, -1, 2)]
        names += [("B2", m, i, -1) for i in ("own", 1, -1, -2)]
        names += [("S", m, i) for i in range(6)]
        names += [("PR", m)]
    for part in range(2):
        names += [("CP", part)]
        for d in (1, -1):
            names += [("C", part, d, k) for k in range(2)]
            names += [("CF", part, d), ("CN", part, d), ("CQ", part, d)]
    return {name: i for i, name in enumerate(names)}


SEMS = semaphore_table()


def gather_kernel(
    bmap, vrows, gen, diag, coup, parent, front, g, cd, gp, gv, dv, cw, sb, pb, pt, lsem, fsem, ssem, rsem
):
    r = lax.axis_index("row")
    t = lax.axis_index("col")
    y, c = r // CORES, r % CORES
    z, x = t // SIDE, t % SIDE
    other = 1 - c
    partner = (y * CORES + other, t)
    pos = [(x, z), (z, x)]

    def wrap(v):
        return (v + 8) % 4

    def ydev(step, core):
        return (wrap(y + step) * CORES + core, t)

    def dev(m, dp, dq):
        p, q = wrap(pos[m][0] + dp), wrap(pos[m][1] + dq)
        return (r, q * SIDE + p) if m == 0 else (r, p * SIDE + q)

    def strip(m, dp, dq):
        return wrap(pos[m][1] + dq) * SIDE + wrap(pos[m][0] + dp)

    own_strip = [strip(0, 0, 0), strip(1, 0, 0)]
    load_strips = [
        pltpu.make_async_copy(gen.at[:, pl.ds(own_strip[m] * STRIP, STRIP), :], gp.at[m], lsem.at[m])
        for m in range(2)
    ]
    load_gen = pltpu.make_async_copy(gen, gv, lsem.at[2])
    load_diag = pltpu.make_async_copy(diag, dv, lsem.at[3])
    load_coup = pltpu.make_async_copy(coup, cw, lsem.at[4])
    load_front = [
        pltpu.make_async_copy(parent.at[a, :, band, 0, :], front.at[a, band], fsem.at[a * BANDS + band])
        for a in range(8) for band in range(BANDS)
    ]
    for load in load_strips:
        load.start()

    barrier = pltpu.get_barrier_semaphore()
    peers = [ydev(s, k) for s in (1, 2, 3) for k in range(CORES)] + [partner]
    peers += [dev(0, s, 0) for s in (1, -1)] + [dev(1, s, 0) for s in (1, -1)]
    for peer in peers:
        pl.semaphore_signal(barrier, inc=1, device_id=peer, device_id_type=MESH)
    load_gen.start()
    load_diag.start()
    load_coup.start()

    entries = [bmap[c, y * GROUP + i] for i in range(GROUP)]

    def source(slot):
        at = y * WINDOW + slot
        before = jnp.int32(0)
        for e in entries:
            before = before + jnp.where(e < at, 1, 0).astype(jnp.int32)
        index = jnp.minimum(before, GROUP - 1)
        there = bmap[c, y * GROUP + index] == at
        return index, jnp.where(there, vrows[c, y * GROUP + index], 0)

    zero = jnp.zeros((), jnp.bfloat16)
    down = lax.broadcasted_iota(jnp.int32, (BLK, BLK), 0)

    for load in load_strips:
        load.wait()
    for m in range(2):
        for d in (2, 1, 3):
            for k in range(CORES):
                index, count = source(m * 8 + CORES * wrap(y - d) + k)
                inside = down[:STRIP] + own_strip[m] * STRIP < count
                sb[m, (d - 1) * CORES + k] = jnp.where(inside, gp[m, index], zero)

    pl.semaphore_wait(barrier, len(peers))

    sent = []

    def send(name, src, dst, to, recv=None):
        k = SEMS[name]
        copy = pltpu.make_async_remote_copy(
            src_ref=src, dst_ref=dst, send_sem=ssem.at[k], recv_sem=rsem.at[k if recv is None else recv],
            device_id=to, device_id_type=MESH,
        )
        copy.start()
        sent.append(copy)

    def arrived(name, ref):
        k = SEMS[name]
        pltpu.make_async_remote_copy(
            src_ref=ref, dst_ref=ref, send_sem=ssem.at[k], recv_sem=rsem.at[k],
            device_id=partner, device_id_type=MESH,
        ).wait_recv()

    for d in (2, 1, 3):
        for m in range(2):
            for k in range(CORES):
                i = (d - 1) * CORES + k
                send(
                    ("S", m, i), sb.at[m, i], g.at[m, own_strip[m], d, c],
                    ydev(-d, k), SEMS[("S", m, 0)] + (d - 1) * CORES + c,
                )
    load_gen.wait()
    index, wanted = source(t)
    cd[c, y, 0] = jnp.where(down < wanted, gv[index], zero)
    for m in range(2):
        index, count = source(m * 8 + y * CORES + other)
        pb[m] = jnp.where(down < count, gv[index], zero).reshape(STRIPS, STRIP, BLK)

    def rows_of(k):
        return pl.ds(k * HALF, HALF)

    def onward(d):
        return 0 if d == 1 else 1

    def send_own(part, lead):
        for d in (1, -1):
            k = onward(d) if lead else 1 - onward(d)
            ref = cd.at[c, y, part, rows_of(k)]
            send(("C", part, d, k), ref, ref, ydev(d, c))

    send_own(0, True)
    send_own(0, False)
    send(("CP", 0), cd.at[c, y, 0], cd.at[c, y, 0], partner)
    for m in range(2):
        send(("PR", m), pb.at[m], g.at[m, :, 0, c], partner)
        index, count = source(m * 8 + r)
        g[m, :, 0, c] = jnp.where(down < count, gv[index], zero).reshape(STRIPS, STRIP, BLK)
    load_diag.wait()
    across = lax.broadcasted_iota(jnp.int32, (BLK, BLK), 1)
    index, count = source(t)
    cd[c, y, 1] = jnp.where(jnp.logical_and(down < count, across < count), dv[index], zero)
    for load in load_front:
        load.start()
    send_own(1, True)
    load_coup.wait()
    for child in range(2):
        cw[child] = cw[child].T

    def piece(m, dp, dq, part=None):
        at = strip(m, dp, dq)
        if part is None:
            return g.at[m, at, pl.ds(1, 3)]
        return g.at[m, at, pl.ds(1, 3), part]

    def item_ref(m, item, dq):
        if item == "own":
            return piece(m, 0, dq)
        if item in (1, -1):
            return piece(m, item, dq)
        return piece(m, 2, dq, 0 if item == 2 else 1)

    def half_ref(m, item, dq, part):
        if item == "own":
            return piece(m, 0, dq, part)
        if item in (1, -1):
            return piece(m, item, dq, part)
        return piece(m, 2, dq, part)

    def first_q(m, item):
        for d in (1, -1):
            ref = item_ref(m, item, 0)
            send(("B1", m, item, d), ref, ref, dev(m, 0, d))

    def second_q(m, item):
        for d in (1, -1):
            arrived(("B1", m, item, d), item_ref(m, item, -d))
            ref = half_ref(m, item, -d, onward(d))
            send(("B2", m, item, d), ref, ref, dev(m, 0, d))

    def second_q_far(m):
        for d in (1, -1):
            for item in (2, -2):
                arrived(("B1", m, item, d), item_ref(m, item, -d))
        for d in (1, -1):
            item = 2 * d
            ref = item_ref(m, item, -d)
            send(("B2", m, item, d), ref, ref, dev(m, 0, d))

    def relay(part):
        for d in (1, -1):
            k = onward(d)
            half = cd.at[c, wrap(y - d), part, rows_of(k)]
            arrived(("C", part, d, k), half)
            send(("CF", part, d), half, half, ydev(d, c))

    def near(part):
        for d in (1, -1):
            k = 1 - onward(d)
            arrived(("C", part, d, k), cd.at[c, wrap(y - d), part, rows_of(k)])
            ref = cd.at[c, wrap(y - d), part]
            send(("CN", part, d), ref, ref, partner)

    def far(part):
        for d in (1, -1):
            half = cd.at[c, wrap(y + 2), part, rows_of(onward(d))]
            arrived(("CF", part, d), half)
            send(("CQ", part, d), half, half, partner)

    def partner_own(part):
        arrived(("CP", part), cd.at[other, y, part])

    def partner_near(part):
        for d in (1, -1):
            arrived(("CN", part, d), cd.at[other, wrap(y - d), part])

    def partner_far(part):
        for d in (1, -1):
            arrived(("CQ", part, d), cd.at[other, wrap(y + 2), part, rows_of(onward(d))])

    def project(s):
        for child in range(2):
            proj = lax.dot_general(
                cw[child], cd[child, s, 0], (((1,), (1,)), ((), ())), preferred_element_type=jnp.float32
            )
            pt[s, child] = proj.astype(jnp.bfloat16)

    def multiply(left, b):
        tile = jnp.dot(left[0], pt[b, 0], preferred_element_type=jnp.float32)
        return tile + jnp.dot(left[1], pt[b, 1], preferred_element_type=jnp.float32)

    def add_to(a, first, rows, b, tile):
        at = pl.ds(first, rows)
        for side in range(2):
            band = side * CHIPS + b
            front[a, band, at] = front[a, band, at] + tile[:, side * LANES:(side + 1) * LANES]

    def own_tiles(b):
        for m in range(2):
            left = [g[m, :, 0, child].reshape(BLK, BLK) for child in range(2)]
            add_to(2 * y + m, 0, BLK, b, multiply(left, b))

    def quarter(m, dq):
        line = z * (1 - m) + x * m
        first = SIDE * wrap(line + dq)
        left = [g[m, pl.ds(first, SIDE), 1:CHIPS, child].reshape(3 * SIDE * STRIP, BLK) for child in range(2)]
        for b in range(CHIPS):
            tile = multiply(left, b)
            for n in range(SIDE):
                for d in (1, 2, 3):
                    at = (n * 3 + d - 1) * STRIP
                    add_to(2 * wrap(y + d) + m, (first + n) * STRIP, STRIP, b, tile[at:at + STRIP])

    def add_diagonals():
        for b in range(CHIPS):
            total = cd[0, b, 1].astype(jnp.float32) + cd[1, b, 1].astype(jnp.float32)
            add_to(2 * b + t // 8, 0, BLK, b, total)

    for d in (1, 3):
        for m in range(2):
            for k in range(CORES):
                arrived(("S", m, (d - 1) * CORES + k), g.at[m, own_strip[m], d, k])
    for m in range(2):
        for k in range(CORES):
            arrived(("S", m, CORES + k), g.at[m, own_strip[m], 2, k])
    for m in range(2):
        for d in (1, -1):
            ref = piece(m, 0, 0)
            send(("A1", m, d), ref, ref, dev(m, d, 0))
    for m in range(2):
        first_q(m, "own")
    send(("CP", 1), cd.at[c, y, 1], cd.at[c, y, 1], partner)
    relay(0)
    send_own(1, False)
    near(0)
    for m in range(2):
        for d in (1, -1):
            arrived(("A1", m, d), piece(m, -d, 0))
            ref = piece(m, -d, 0, onward(d))
            send(("A2", m, d), ref, ref, dev(m, d, 0))
        for d in (1, -1):
            first_q(m, -d)
    for m in range(2):
        second_q(m, "own")
    relay(1)
    partner_own(0)
    partner_near(0)
    for load in load_front:
        load.wait()
    for m in range(2):
        arrived(("PR", m), g.at[m, :, 0, other])

    @pl.loop(0, 3)
    def _(i):
        project(wrap(y + i - 1))

    for m in range(2):
        for d in (1, -1):
            arrived(("A2", m, d), piece(m, 2, 0, onward(d)))
            first_q(m, 2 * d)
    far(0)

    @pl.loop(0, 3)
    def _(i):
        own_tiles(wrap(y + i - 1))

    for m in range(2):
        for d in (1, -1):
            second_q(m, d)
    near(1)
    partner_far(0)
    project(wrap(y + 2))
    own_tiles(wrap(y + 2))
    for m in range(2):
        second_q_far(m)
    far(1)

    @pl.loop(0, 6)
    def _(i):
        quarter(i // 3, i % 3 - 1)

    partner_own(1)
    partner_near(1)
    partner_far(1)

    @pl.when(r == t % 8)
    def _():
        add_diagonals()

    for m in range(2):
        for d in (1, -1):
            for item in ("own", 1, -1, 2 * d):
                arrived(("B2", m, item, d), half_ref(m, item, 2, onward(d)))

    @pl.loop(0, 2)
    def _(m):
        quarter(m, 2)

    for copy in sent:
        copy.wait_send()


def write_kernel(front, out, sems):
    copies = [
        pltpu.make_async_copy(front.at[a, band], out.at[a, :, band, 0, :], sems.at[a * BANDS + band])
        for a in range(8) for band in range(BANDS)
    ]
    for copy in copies:
        copy.start()
    for copy in copies:
        copy.wait()


def shards(parent_front, generators, diagonal_blocks, coupling, block_map, valid_rows):
    banded = parent_front.reshape(8, BLK, CHIPS, 2, LANES).transpose(0, 1, 3, 2, 4).reshape(8, BLK, BANDS, 1, LANES)
    any_spec = pl.BlockSpec(memory_space=pl.ANY)
    vmem = pl.BlockSpec(memory_space=pltpu.VMEM)
    smem = pl.BlockSpec(memory_space=pltpu.SMEM)
    bf16 = jnp.bfloat16
    front = pl.pallas_call(
        gather_kernel,
        name="gather",
        in_specs=[smem, smem, any_spec, any_spec, any_spec, any_spec],
        out_specs=vmem,
        out_shape=pltpu.VMEM((8, BANDS, BLK, LANES), jnp.float32),
        scratch_shapes=[
            pltpu.VMEM((2, STRIPS, CHIPS, 2, STRIP, BLK), bf16),
            pltpu.VMEM((2, CHIPS, 2, BLK, BLK), bf16),
            pltpu.VMEM((2, GROUP, STRIP, BLK), bf16),
            pltpu.VMEM((GROUP, BLK, BLK), bf16),
            pltpu.VMEM((GROUP, BLK, BLK), bf16),
            pltpu.VMEM((2, BLK, BLK), bf16),
            pltpu.VMEM((2, 6, STRIP, BLK), bf16),
            pltpu.VMEM((2, STRIPS, STRIP, BLK), bf16),
            pltpu.VMEM((CHIPS, 2, BLK, BLK), bf16),
            pltpu.SemaphoreType.DMA((5,)),
            pltpu.SemaphoreType.DMA((8 * BANDS,)),
            pltpu.SemaphoreType.DMA((len(SEMS),)),
            pltpu.SemaphoreType.DMA((len(SEMS),)),
        ],
        compiler_params=pltpu.CompilerParams(
            collective_id=0, has_side_effects=True, vmem_limit_bytes=52 << 20
        ),
    )(block_map, valid_rows, generators, diagonal_blocks, coupling, banded)
    out = pl.pallas_call(
        write_kernel,
        name="write",
        in_specs=[vmem],
        out_specs=any_spec,
        out_shape=jax.ShapeDtypeStruct((8, BLK, BANDS, 1, LANES), jnp.float32),
        scratch_shapes=[pltpu.SemaphoreType.DMA((8 * BANDS,))],
        compiler_params=pltpu.CompilerParams(vmem_limit_bytes=1 << 20),
    )(front)
    return out.reshape(8, BLK, 2, CHIPS, LANES).transpose(0, 1, 3, 2, 4).reshape(8, BLK, CHIPS, BLK)


def solution(mesh):
    in_specs = (
        P(None, "row", None, "col"),
        P("row", None, None),
        P("row", None, None),
        P(),
        P(),
        P(),
    )
    out_specs = P(None, "row", None, "col")
    return jax.shard_map(shards, mesh=mesh, in_specs=in_specs, out_specs=out_specs, check_vma=False)
```

```python
import math

import jax
import jax.numpy as jnp
from jax import lax
from jax.experimental import pallas as pl
from jax.experimental.pallas import tpu as pltpu
from jax.sharding import PartitionSpec as P

MESH = pl.DeviceIdType.MESH
CHIPS = 4
CORES = 2
SIDE = 4
GROUP = 12
WINDOW = 16
STRIPS = 16
BLK = 256
STRIP = BLK // STRIPS
LANES = 128
HALF = BLK // 2
BANDS = 8


def arrival_groups():
    names = ["S", "PR", "P0", "N0", "Q0", "P1"]
    for m in range(2):
        names += [("A1", m), ("A2", m), ("B1", m, 0), ("B1", m, 1), ("B1", m, 2), ("B2", m)]
    for part in range(2):
        names += [("CL", part), ("CO", part), ("CF", part)]
    return {name: i for i, name in enumerate(names)}


GROUPS = arrival_groups()


def product(left, pt, b):
    tile = jnp.dot(left[0], pt[b, 0], preferred_element_type=jnp.float32)
    return tile + jnp.dot(left[1], pt[b, 1], preferred_element_type=jnp.float32)


def add_block(front, a, first, rows, b, tile):
    at = pl.ds(first, rows)
    for side in range(2):
        band = side * CHIPS + b
        front[a, band, at] = front[a, band, at] + tile[:, side * LANES:(side + 1) * LANES]


def quarter_rows(g, m, first):
    return [g[m, pl.ds(first, SIDE), 1:CHIPS, child].reshape(3 * SIDE * STRIP, BLK) for child in range(2)]


def add_quarter(front, y, m, first, b, tile):
    for n in range(SIDE):
        for d in (1, 2, 3):
            at = (n * 3 + d - 1) * STRIP
            add_block(front, 2 * ((y + d) % CHIPS) + m, (first + n) * STRIP, STRIP, b, tile[at:at + STRIP])


def gather_kernel(
    maps, counts, gen, diag, coup, parent, front, g, pt, bmap, vrows, cd, gp, gv, dv, cw, sb, pb, lsem, ssem, rsem
):
    r = lax.axis_index("row")
    t = lax.axis_index("col")
    y, c = r // CORES, r % CORES
    z, x = t // SIDE, t % SIDE
    other = 1 - c
    partner = (y * CORES + other, t)
    pos = [(x, z), (z, x)]

    def wrap(v):
        return (v + 8) % 4

    def ydev(step, core):
        return (wrap(y + step) * CORES + core, t)

    def dev(m, dp, dq):
        p, q = wrap(pos[m][0] + dp), wrap(pos[m][1] + dq)
        return (r, q * SIDE + p) if m == 0 else (r, p * SIDE + q)

    def strip(m, dp, dq):
        return wrap(pos[m][1] + dq) * SIDE + wrap(pos[m][0] + dp)

    barrier = pltpu.get_barrier_semaphore()
    peers = [ydev(s, k) for s in (2, 1, 3) for k in range(CORES)] + [partner]
    peers += [dev(m, s, 0) for s in (2, 1, -1) for m in range(2)]
    for peer in peers:
        pl.semaphore_signal(barrier, inc=1, device_id=peer, device_id_type=MESH)

    own_strip = [strip(0, 0, 0), strip(1, 0, 0)]
    load_strips = [
        pltpu.make_async_copy(gen.at[:, pl.ds(own_strip[m] * STRIP, STRIP), :], gp.at[m], lsem.at[0])
        for m in range(2)
    ]
    load_tables = [pltpu.make_async_copy(maps, bmap, lsem.at[1]), pltpu.make_async_copy(counts, vrows, lsem.at[2])]
    load_gen = pltpu.make_async_copy(gen, gv, lsem.at[3])
    load_diag = pltpu.make_async_copy(diag, dv, lsem.at[4])
    load_coup = pltpu.make_async_copy(coup, cw, lsem.at[5])
    load_front = [
        pltpu.make_async_copy(parent.at[a, :, band, 0, :], front.at[a, band], lsem.at[6])
        for a in range(8) for band in range(BANDS)
    ]
    for load in load_strips + load_tables + [load_gen, load_diag, load_coup]:
        load.start()
    zero = jnp.zeros((), jnp.bfloat16)
    down = lax.broadcasted_iota(jnp.int32, (BLK, BLK), 0)
    pltpu.make_async_copy(gp, gp, lsem.at[0]).wait()
    for load in load_tables:
        load.wait()

    entries = [bmap[c, y * GROUP + i] for i in range(GROUP)]

    def source(slot):
        at = y * WINDOW + slot
        before = jnp.int32(0)
        for e in entries:
            before = before + jnp.where(e < at, 1, 0).astype(jnp.int32)
        index = jnp.minimum(before, GROUP - 1)
        there = bmap[c, y * GROUP + index] == at
        return index, jnp.where(there, vrows[c, y * GROUP + index], 0)

    for m in range(2):
        for d in (2, 1, 3):
            for k in range(CORES):
                index, count = source(m * 8 + CORES * wrap(y - d) + k)
                inside = down[:STRIP] + own_strip[m] * STRIP < count
                sb[m, (d - 1) * CORES + k] = jnp.where(inside, gp[m, index], zero)

    pl.semaphore_wait(barrier, len(peers))

    sent = []

    def send(group, src, dst, to):
        copy = pltpu.make_async_remote_copy(
            src_ref=src, dst_ref=dst, send_sem=ssem, recv_sem=rsem.at[GROUPS[group]],
            device_id=to, device_id_type=MESH,
        )
        copy.start()
        sent.append(math.prod(src.shape))

    def arrived(group, size):
        pltpu.make_async_remote_copy(
            src_ref=size, dst_ref=size, send_sem=ssem, recv_sem=rsem.at[GROUPS[group]],
            device_id=partner, device_id_type=MESH,
        ).wait_recv()

    for d in (2, 1, 3):
        for m in range(2):
            for k in range(CORES):
                i = (d - 1) * CORES + k
                send("S", sb.at[m, i], g.at[m, own_strip[m], d, c], ydev(-d, k))
    load_gen.wait()
    index, wanted = source(t)
    cd[c, y, 0] = jnp.where(down < wanted, gv[index], zero)
    for m in range(2):
        index, count = source(m * 8 + y * CORES + other)
        pb[m] = jnp.where(down < count, gv[index], zero).reshape(STRIPS, STRIP, BLK)

    def rows_of(k):
        return pl.ds(k * HALF, HALF)

    def onward(d):
        return 0 if d == 1 else 1

    def send_own(part, lead):
        for d in (1, -1):
            k = onward(d) if lead else 1 - onward(d)
            ref = cd.at[c, y, part, rows_of(k)]
            send(("CL" if lead else "CO", part), ref, ref, ydev(d, c))

    send_own(0, True)
    send_own(0, False)
    send("P0", cd.at[c, y, 0], cd.at[c, y, 0], partner)
    for m in range(2):
        send("PR", pb.at[m], g.at[m, :, 0, c], partner)
        index, count = source(m * 8 + r)
        g[m, :, 0, c] = jnp.where(down < count, gv[index], zero).reshape(STRIPS, STRIP, BLK)
    load_diag.wait()
    across = lax.broadcasted_iota(jnp.int32, (BLK, BLK), 1)
    index, count = source(t)
    cd[c, y, 1] = jnp.where(jnp.logical_and(down < count, across < count), dv[index], zero)
    for load in load_front:
        load.start()
    send_own(1, True)
    load_coup.wait()
    for child in range(2):
        cw[child] = cw[child].T

    def piece(m, dp, dq, part=None):
        at = strip(m, dp, dq)
        if part is None:
            return g.at[m, at, pl.ds(1, 3)]
        return g.at[m, at, pl.ds(1, 3), part]

    def first_q(m, item):
        for d in (1, -1):
            ref = piece(m, item, 0)
            send(("B1", m, abs(item)), ref, ref, dev(m, 0, d))

    def second_q(m, items):
        arrived(("B1", m, abs(items[0])), g.at[m, pl.ds(0, 2 * len(items)), pl.ds(1, 3)])
        for item in items:
            for d in (1, -1):
                ref = piece(m, item, -d, onward(d))
                send(("B2", m), ref, ref, dev(m, 0, d))

    one_block = cd.at[0, 0, 0]

    def relay(part):
        arrived(("CL", part), one_block)
        for d in (1, -1):
            half = cd.at[c, wrap(y - d), part, rows_of(onward(d))]
            send(("CF", part), half, half, ydev(d, c))

    def near(part):
        arrived(("CO", part), one_block)
        for d in (1, -1):
            ref = cd.at[c, wrap(y - d), part]
            send(("N0", "P1")[part], ref, ref, partner)

    def far(part):
        arrived(("CF", part), one_block)
        for d in (1, -1):
            half = cd.at[c, wrap(y + 2), part, rows_of(onward(d))]
            send(("Q0", "P1")[part], half, half, partner)

    def project(s):
        for child in range(2):
            proj = lax.dot_general(
                cw[child], cd[child, s, 0], (((1,), (1,)), ((), ())), preferred_element_type=jnp.float32
            )
            pt[s, child] = proj.astype(jnp.bfloat16)

    def add_to(a, first, rows, b, tile):
        add_block(front, a, first, rows, b, tile)

    def multiply(left, b):
        return product(left, pt, b)

    def own_tiles(b):
        for m in range(2):
            left = [g[m, :, 0, child].reshape(BLK, BLK) for child in range(2)]
            add_to(2 * y + m, 0, BLK, b, multiply(left, b))

    def quarter(m, dq):
        first = SIDE * wrap(z * (1 - m) + x * m + dq)
        left = quarter_rows(g, m, first)
        for b in range(CHIPS):
            add_quarter(front, y, m, first, b, multiply(left, b))

    def add_diagonals():
        for b in range(CHIPS):
            total = cd[0, b, 1].astype(jnp.float32) + cd[1, b, 1].astype(jnp.float32)
            add_to(2 * b + t // 8, 0, BLK, b, total)

    arrived("P0", one_block)
    project(y)
    arrived("PR", g.at[:, :, 0, 0])
    arrived("S", g.at[0, pl.ds(0, 2), pl.ds(1, 3)])
    for m in range(2):
        ref = piece(m, 0, 0)
        for d in (1, -1):
            send(("A1", m), ref, ref, dev(m, d, 0))
        send(("A2", m), ref, ref, dev(m, 2, 0))
    for m in range(2):
        first_q(m, 0)
    send("P1", cd.at[c, y, 1], cd.at[c, y, 1], partner)
    relay(0)
    send_own(1, False)
    pltpu.make_async_copy(front, front, lsem.at[6]).wait()
    own_tiles(y)
    near(0)
    for m in range(2):
        arrived(("A1", m), g.at[m, pl.ds(0, 2), pl.ds(1, 3)])
        for d in (1, -1):
            first_q(m, -d)
    for m in range(2):
        second_q(m, (0,))
    far(0)
    for m in range(2):
        arrived(("A2", m), g.at[m, 0, pl.ds(1, 3)])
        first_q(m, 2)
    relay(1)
    near(1)
    arrived("N0", cd.at[0, pl.ds(0, 2), 0])

    @pl.loop(0, 2)
    def _(i):
        project(wrap(y + 2 * i - 1))

    for m in range(2):
        second_q(m, (1, -1))

    @pl.loop(0, 2)
    def _(i):
        own_tiles(wrap(y + 2 * i - 1))

    for m in range(2):
        second_q(m, (2,))
    arrived("Q0", one_block)
    project(wrap(y + 2))
    own_tiles(wrap(y + 2))

    @pl.loop(0, 2)
    def _(m):
        quarter(m, 0)

    far(1)

    @pl.loop(0, 4)
    def _(i):
        quarter(i // 2, 2 * (i % 2) - 1)

    arrived("P1", cd.at[0, :, 1])

    @pl.when(r == t % 8)
    def _():
        add_diagonals()

    for m in range(2):
        arrived(("B2", m), g.at[m, pl.ds(0, 4), pl.ds(1, 3)])
    blocks, rest = divmod(sum(sent), 2 * CHIPS * BLK * LANES)
    assert rest == 0
    everything = front.at[pl.ds(0, blocks), pl.ds(0, CHIPS)]
    pltpu.make_async_remote_copy(
        src_ref=everything, dst_ref=everything, send_sem=ssem, recv_sem=rsem.at[0],
        device_id=partner, device_id_type=MESH,
    ).wait_send()


def write_kernel(taken, g, pt, out, front, done):
    y = lax.axis_index("row") // CORES
    t = lax.axis_index("col")
    lines = [t // SIDE, t % SIDE]

    def write(a, b):
        for side in range(2):
            band = side * CHIPS + b
            pltpu.make_async_copy(front.at[a, band], out.at[a, :, band, 0, :], done).start()

    for m in range(2):
        for b in range(CHIPS):
            write(2 * y + m, b)
    for m in range(2):
        first = SIDE * ((lines[m] + 2) % SIDE)
        left = quarter_rows(g, m, first)
        for b in range(CHIPS):
            add_quarter(front, y, m, first, b, product(left, pt, b))
            for d in (1, 2, 3):
                write(2 * ((y + d) % CHIPS) + m, b)
    pltpu.make_async_copy(front, front, done).wait()


def shards(parent_front, generators, diagonal_blocks, coupling, block_map, valid_rows):
    banded = parent_front.reshape(8, BLK, CHIPS, 2, LANES).transpose(0, 1, 3, 2, 4).reshape(8, BLK, BANDS, 1, LANES)
    any_spec = pl.BlockSpec(memory_space=pl.ANY)
    vmem = pl.BlockSpec(memory_space=pltpu.VMEM)
    bf16 = jnp.bfloat16
    front_shape = pltpu.VMEM((8, BANDS, BLK, LANES), jnp.float32)
    front, g, pt = pl.pallas_call(
        gather_kernel,
        name="gather",
        in_specs=[any_spec] * 6,
        out_specs=[vmem] * 3,
        out_shape=[
            front_shape,
            pltpu.VMEM((2, STRIPS, CHIPS, 2, STRIP, BLK), bf16),
            pltpu.VMEM((CHIPS, 2, BLK, BLK), bf16),
        ],
        scratch_shapes=[
            pltpu.SMEM(block_map.shape, jnp.int32),
            pltpu.SMEM(valid_rows.shape, jnp.int32),
            pltpu.VMEM((2, CHIPS, 2, BLK, BLK), bf16),
            pltpu.VMEM((2, GROUP, STRIP, BLK), bf16),
            pltpu.VMEM((GROUP, BLK, BLK), bf16),
            pltpu.VMEM((GROUP, BLK, BLK), bf16),
            pltpu.VMEM((2, BLK, BLK), bf16),
            pltpu.VMEM((2, 6, STRIP, BLK), bf16),
            pltpu.VMEM((2, STRIPS, STRIP, BLK), bf16),
            pltpu.SemaphoreType.DMA((7,)),
            pltpu.SemaphoreType.DMA,
            pltpu.SemaphoreType.DMA((len(GROUPS),)),
        ],
        compiler_params=pltpu.CompilerParams(
            collective_id=0, has_side_effects=True, vmem_limit_bytes=52 << 20
        ),
    )(block_map, valid_rows, generators, diagonal_blocks, coupling, banded)
    out, _ = pl.pallas_call(
        write_kernel,
        name="write",
        in_specs=[vmem] * 3,
        out_specs=[any_spec, vmem],
        out_shape=[jax.ShapeDtypeStruct((8, BLK, BANDS, 1, LANES), jnp.float32), front_shape],
        input_output_aliases={0: 1},
        scratch_shapes=[pltpu.SemaphoreType.DMA],
        compiler_params=pltpu.CompilerParams(vmem_limit_bytes=2 << 20),
    )(front, g, pt)
    return out.reshape(8, BLK, 2, CHIPS, LANES).transpose(0, 1, 3, 2, 4).reshape(8, BLK, CHIPS, BLK)


def solution(mesh):
    in_specs = (
        P(None, "row", None, "col"),
        P("row", None, None),
        P("row", None, None),
        P(),
        P(),
        P(),
    )
    out_specs = P(None, "row", None, "col")
    return jax.shard_map(shards, mesh=mesh, in_specs=in_specs, out_specs=out_specs, check_vma=False)
```

```python
import math

import jax
import jax.numpy as jnp
from jax import lax
from jax.experimental import pallas as pl
from jax.experimental.pallas import tpu as pltpu
from jax.sharding import PartitionSpec as P

MESH = pl.DeviceIdType.MESH
CHIPS = 4
CORES = 2
SIDE = 4
GROUP = 12
WINDOW = 16
STRIPS = 16
BLK = 256
STRIP = BLK // STRIPS
LANES = 128
HALF = BLK // 2
BANDS = 8


def arrival_groups():
    names = ["S", "SF", "PR", "P0", "N0", "Q0", "CL", "CO", "CF", "DX", "DD"]
    for m in range(2):
        names += [("A1", m), ("A2", m), ("B1", m, 0), ("B1", m, 1), ("B1", m, 2), ("B2", m)]
    return {name: i for i, name in enumerate(names)}


GROUPS = arrival_groups()


def product(left, pt, b):
    tile = jnp.dot(left[0], pt[b, 0], preferred_element_type=jnp.float32)
    return tile + jnp.dot(left[1], pt[b, 1], preferred_element_type=jnp.float32)


def add_block(front, a, first, rows, b, tile):
    at = pl.ds(first, rows)
    for side in range(2):
        band = side * CHIPS + b
        front[a, band, at] = front[a, band, at] + tile[:, side * LANES:(side + 1) * LANES]


def quarter_rows(g, m, first):
    return [g[m, pl.ds(first, SIDE), 1:CHIPS, child].reshape(3 * SIDE * STRIP, BLK) for child in range(2)]


def add_quarter(front, y, m, first, b, tile):
    for n in range(SIDE):
        for d in (1, 2, 3):
            at = (n * 3 + d - 1) * STRIP
            add_block(front, 2 * ((y + d) % CHIPS) + m, (first + n) * STRIP, STRIP, b, tile[at:at + STRIP])


def gather_kernel(
    maps, counts, gen, diag, coup, parent, front, g, pt,
    bmap, vrows, cd, gp, gv, dv, cw, sb, sf, pb, dm, dx, dc, dd, lsem, ssem, dsem, rsem
):
    r = lax.axis_index("row")
    t = lax.axis_index("col")
    y, c = r // CORES, r % CORES
    z, x = t // SIDE, t % SIDE
    other = 1 - c
    partner = (y * CORES + other, t)
    pos = [(x, z), (z, x)]

    def wrap(v):
        return (v + 8) % 4

    def ydev(step, core):
        return (wrap(y + step) * CORES + core, t)

    def dev(m, dp, dq):
        p, q = wrap(pos[m][0] + dp), wrap(pos[m][1] + dq)
        return (r, q * SIDE + p) if m == 0 else (r, p * SIDE + q)

    def strip(m, dp, dq):
        return wrap(pos[m][1] + dq) * SIDE + wrap(pos[m][0] + dp)

    barrier = pltpu.get_barrier_semaphore()
    peers = [ydev(s, k) for s in (2, 1, 3) for k in range(CORES)] + [partner]
    peers += [dev(m, s, 0) for s in (1, -1) for m in range(2)]
    for peer in peers:
        pl.semaphore_signal(barrier, inc=1, device_id=peer, device_id_type=MESH)

    own_strip = [strip(0, 0, 0), strip(1, 0, 0)]
    load_strips = [
        pltpu.make_async_copy(gen.at[:, pl.ds(own_strip[m] * STRIP, STRIP), :], gp.at[m], lsem.at[0])
        for m in range(2)
    ]
    load_tables = [pltpu.make_async_copy(maps, bmap, lsem.at[1]), pltpu.make_async_copy(counts, vrows, lsem.at[2])]
    load_gen = pltpu.make_async_copy(gen, gv, lsem.at[3])
    load_diag = pltpu.make_async_copy(diag, dv, lsem.at[4])
    load_coup = pltpu.make_async_copy(coup, cw, lsem.at[5])
    load_front = [
        pltpu.make_async_copy(parent.at[a, :, band, 0, :], front.at[a, band], lsem.at[6])
        for a in range(8) for band in range(BANDS)
    ]
    for load in load_strips + load_tables + [load_gen, load_diag, load_coup]:
        load.start()
    zero = jnp.zeros((), jnp.bfloat16)
    down = lax.broadcasted_iota(jnp.int32, (BLK, BLK), 0)
    pltpu.make_async_copy(gp, gp, lsem.at[0]).wait()
    for load in load_tables:
        load.wait()

    entries = [bmap[c, y * GROUP + i] for i in range(GROUP)]

    def source(slot):
        at = y * WINDOW + slot
        before = jnp.int32(0)
        for e in entries:
            before = before + jnp.where(e < at, 1, 0).astype(jnp.int32)
        index = jnp.minimum(before, GROUP - 1)
        there = bmap[c, y * GROUP + index] == at
        return index, jnp.where(there, vrows[c, y * GROUP + index], 0)

    for m in range(2):
        for d in (2, 1, 3):
            for k in range(CORES):
                index, count = source(m * 8 + CORES * wrap(y - d) + k)
                inside = down[:STRIP] + own_strip[m] * STRIP < count
                sb[m, (d - 1) * CORES + k] = jnp.where(inside, gp[m, index], zero)

    pl.semaphore_wait(barrier, len(peers))

    sent = [0, 0]

    def send(group, src, dst, to):
        plane = int(isinstance(group, tuple))
        copy = pltpu.make_async_remote_copy(
            src_ref=src, dst_ref=dst, send_sem=ssem.at[plane], recv_sem=rsem.at[GROUPS[group]],
            device_id=to, device_id_type=MESH,
        )
        copy.start()
        sent[plane] += math.prod(src.shape)

    def arrived(group, size):
        pltpu.make_async_remote_copy(
            src_ref=size, dst_ref=size, send_sem=ssem.at[0], recv_sem=rsem.at[GROUPS[group]],
            device_id=partner, device_id_type=MESH,
        ).wait_recv()

    for d in (2, 1, 3):
        for m in range(2):
            for k in range(CORES):
                i = (d - 1) * CORES + k
                send("S", sb.at[m, i], g.at[m, own_strip[m], d, c], ydev(-d, k))
    load_gen.wait()
    index, wanted = source(t)
    cd[c, y] = jnp.where(down < wanted, gv[index], zero)
    for m in range(2):
        index, count = source(m * 8 + y * CORES + other)
        pb[m] = jnp.where(down < count, gv[index], zero).reshape(STRIPS, STRIP, BLK)

    def rows_of(k):
        return pl.ds(k * HALF, HALF)

    def onward(d):
        return 0 if d == 1 else 1

    for lead in (True, False):
        for d in (1, -1):
            half = cd.at[c, y, rows_of(onward(d) if lead else 1 - onward(d))]
            send("CL" if lead else "CO", half, half, ydev(d, c))
    send("P0", cd.at[c, y], cd.at[c, y], partner)
    far_strip = [strip(0, 2, 2), strip(1, 2, 2)]
    for m in range(2):
        send("PR", pb.at[m], g.at[m, :, 0, c], partner)
        index, count = source(m * 8 + r)
        g[m, :, 0, c] = jnp.where(down < count, gv[index], zero).reshape(STRIPS, STRIP, BLK)
        for d in (1, 2, 3):
            for k in range(CORES):
                index, count = source(m * 8 + CORES * wrap(y - d) + k)
                inside = down[:STRIP] + far_strip[m] * STRIP < count
                rows = gv[index, pl.ds(pl.multiple_of(far_strip[m] * STRIP, STRIP), STRIP)]
                sf[m, (d - 1) * CORES + k] = jnp.where(inside, rows, zero)
    load_diag.wait()
    across = lax.broadcasted_iota(jnp.int32, (BLK, BLK), 1)
    index, count = source(t)
    dm[...] = jnp.where(jnp.logical_and(down < count, across < count), dv[index], zero)
    for load in load_front:
        load.start()
    send("DX", dm.at[pl.ds(other * HALF, HALF)], dx, partner)
    load_coup.wait()
    for child in range(2):
        cw[child] = cw[child].T

    def piece(m, dp, dq, part=None):
        at = strip(m, dp, dq)
        if part is None:
            return g.at[m, at, pl.ds(1, 3)]
        return g.at[m, at, pl.ds(1, 3), part]

    def first_q(m, item):
        for d in (1, -1):
            ref = piece(m, item, 0)
            send(("B1", m, abs(item)), ref, ref, dev(m, 0, d))

    def second_q(m, items):
        arrived(("B1", m, abs(items[0])), g.at[m, pl.ds(0, 2 * len(items)), pl.ds(1, 3)])
        for item in items:
            for d in (1, -1):
                ref = piece(m, item, -d, onward(d))
                send(("B2", m), ref, ref, dev(m, 0, d))

    one_block = cd.at[0, 0]

    def project(s):
        for child in range(2):
            proj = lax.dot_general(
                cw[child], cd[child, s], (((1,), (1,)), ((), ())), preferred_element_type=jnp.float32
            )
            pt[s, child] = proj.astype(jnp.bfloat16)

    def add_to(a, first, rows, b, tile):
        add_block(front, a, first, rows, b, tile)

    def multiply(left, b):
        return product(left, pt, b)

    def own_tiles(b):
        for m in range(2):
            left = [g[m, :, 0, child].reshape(BLK, BLK) for child in range(2)]
            add_to(2 * y + m, 0, BLK, b, multiply(left, b))

    def quarter(m, dq):
        first = SIDE * wrap(z * (1 - m) + x * m + dq)
        left = quarter_rows(g, m, first)
        for b in range(CHIPS):
            add_quarter(front, y, m, first, b, multiply(left, b))

    arrived("P0", one_block)
    project(y)
    arrived("DX", dx)
    total = dm[pl.ds(c * HALF, HALF)].astype(jnp.float32) + dx[...].astype(jnp.float32)
    dc[...] = total.astype(jnp.bfloat16)
    arrived("PR", g.at[:, :, 0, 0])

    def diagonal_send():
        return pltpu.make_async_remote_copy(
            src_ref=dc, dst_ref=dd.at[y, pl.ds(c * HALF, HALF)], send_sem=dsem, recv_sem=rsem.at[GROUPS["DD"]],
            device_id=(t % 8, t), device_id_type=MESH,
        )

    arrived("S", g.at[0, pl.ds(0, 2), pl.ds(1, 3)])
    for m in range(2):
        ref = piece(m, 0, 0)
        for d in (1, -1):
            send(("A1", m), ref, ref, dev(m, d, 0))
    for m in range(2):
        first_q(m, 0)
    arrived("CL", one_block)
    for d in (1, -1):
        half = cd.at[c, wrap(y - d), rows_of(onward(d))]
        send("CF", half, half, ydev(d, c))
    for d in (2, 1, 3):
        for m in range(2):
            for k in range(CORES):
                send("SF", sf.at[m, (d - 1) * CORES + k], g.at[m, far_strip[m], d, c], ydev(-d, k))

    @pl.when(r != t % 8)
    def _():
        diagonal_send().start()

    pltpu.make_async_copy(front, front, lsem.at[6]).wait()
    own_tiles(y)
    arrived("CO", one_block)
    for d in (1, -1):
        ref = cd.at[c, wrap(y - d)]
        send("N0", ref, ref, partner)
    for m in range(2):
        arrived(("A1", m), g.at[m, pl.ds(0, 2), pl.ds(1, 3)])
        for d in (1, -1):
            ref = piece(m, -d, 0, onward(d))
            send(("A2", m), ref, ref, dev(m, d, 0))
    for m in range(2):
        for d in (1, -1):
            first_q(m, d)
    for m in range(2):
        second_q(m, (0,))
    arrived("N0", cd.at[0, pl.ds(0, 2)])

    @pl.loop(0, 2)
    def _(i):
        project(wrap(y + 2 * i - 1))

    arrived("CF", one_block)
    for d in (1, -1):
        half = cd.at[c, wrap(y + 2), rows_of(onward(d))]
        send("Q0", half, half, partner)
    for m in range(2):
        arrived(("A2", m), g.at[m, 0, pl.ds(1, 3)])
        first_q(m, 2)

    @pl.loop(0, 2)
    def _(i):
        own_tiles(wrap(y + 2 * i - 1))

    for m in range(2):
        second_q(m, (1, -1))
    arrived("Q0", one_block)
    project(wrap(y + 2))
    own_tiles(wrap(y + 2))

    @pl.loop(0, 2)
    def _(m):
        quarter(m, 0)

    @pl.when(r == t % 8)
    def _():
        dd[y, pl.ds(c * HALF, HALF)] = dc[...]
        arrived("DD", gv.at[pl.ds(0, 7), pl.ds(0, HALF)])
        for b in range(CHIPS):
            add_to(2 * b + t // 8, 0, BLK, b, dd[b].astype(jnp.float32))

    @pl.when(r != t % 8)
    def _():
        diagonal_send().wait_send()

    for m in range(2):
        arrived(("B1", m, 2), g.at[m, pl.ds(0, 2), pl.ds(1, 3)])
    arrived("SF", g.at[0, pl.ds(0, 2), pl.ds(1, 3)])
    for m in range(2):
        arrived(("B2", m), g.at[m, pl.ds(0, 3), pl.ds(1, 3)])
    for plane in range(2):
        rows, rest = divmod(sent[plane], 2 * 2 * BANDS * LANES)
        assert rest == 0 and rows <= BLK and rows % 8 == 0
        size = front.at[pl.ds(0, 2), :, pl.ds(0, rows)]
        pltpu.make_async_remote_copy(
            src_ref=size, dst_ref=size, send_sem=ssem.at[plane], recv_sem=rsem.at[0],
            device_id=partner, device_id_type=MESH,
        ).wait_send()


def write_kernel(taken, g, pt, out, front, done):
    y = lax.axis_index("row") // CORES
    t = lax.axis_index("col")
    lines = [t // SIDE, t % SIDE]

    def write(a, b):
        for side in range(2):
            band = side * CHIPS + b
            pltpu.make_async_copy(front.at[a, band], out.at[a, :, band, 0, :], done).start()

    for m in range(2):
        for b in range(CHIPS):
            write(2 * y + m, b)
    for m in range(2):
        firsts = [SIDE * ((lines[m] + step) % SIDE) for step in (1, 3, 2)]
        lefts = [quarter_rows(g, m, first) for first in firsts]
        for b in range(CHIPS):
            for first, left in zip(firsts, lefts):
                add_quarter(front, y, m, first, b, product(left, pt, b))
            for d in (1, 2, 3):
                write(2 * ((y + d) % CHIPS) + m, b)
    pltpu.make_async_copy(front, front, done).wait()


def shards(parent_front, generators, diagonal_blocks, coupling, block_map, valid_rows):
    banded = parent_front.reshape(8, BLK, CHIPS, 2, LANES).transpose(0, 1, 3, 2, 4).reshape(8, BLK, BANDS, 1, LANES)
    any_spec = pl.BlockSpec(memory_space=pl.ANY)
    vmem = pl.BlockSpec(memory_space=pltpu.VMEM)
    bf16 = jnp.bfloat16
    front_shape = pltpu.VMEM((8, BANDS, BLK, LANES), jnp.float32)
    front, g, pt = pl.pallas_call(
        gather_kernel,
        name="gather",
        in_specs=[any_spec] * 6,
        out_specs=[vmem] * 3,
        out_shape=[
            front_shape,
            pltpu.VMEM((2, STRIPS, CHIPS, 2, STRIP, BLK), bf16),
            pltpu.VMEM((CHIPS, 2, BLK, BLK), bf16),
        ],
        scratch_shapes=[
            pltpu.SMEM(block_map.shape, jnp.int32),
            pltpu.SMEM(valid_rows.shape, jnp.int32),
            pltpu.VMEM((2, CHIPS, BLK, BLK), bf16),
            pltpu.VMEM((2, GROUP, STRIP, BLK), bf16),
            pltpu.VMEM((GROUP, BLK, BLK), bf16),
            pltpu.VMEM((GROUP, BLK, BLK), bf16),
            pltpu.VMEM((2, BLK, BLK), bf16),
            pltpu.VMEM((2, 6, STRIP, BLK), bf16),
            pltpu.VMEM((2, 6, STRIP, BLK), bf16),
            pltpu.VMEM((2, STRIPS, STRIP, BLK), bf16),
            pltpu.VMEM((BLK, BLK), bf16),
            pltpu.VMEM((HALF, BLK), bf16),
            pltpu.VMEM((HALF, BLK), bf16),
            pltpu.VMEM((CHIPS, BLK, BLK), bf16),
            pltpu.SemaphoreType.DMA((7,)),
            pltpu.SemaphoreType.DMA((2,)),
            pltpu.SemaphoreType.DMA,
            pltpu.SemaphoreType.DMA((len(GROUPS),)),
        ],
        compiler_params=pltpu.CompilerParams(
            collective_id=0, has_side_effects=True, vmem_limit_bytes=52 << 20
        ),
    )(block_map, valid_rows, generators, diagonal_blocks, coupling, banded)
    out, _ = pl.pallas_call(
        write_kernel,
        name="write",
        in_specs=[vmem] * 3,
        out_specs=[any_spec, vmem],
        out_shape=[jax.ShapeDtypeStruct((8, BLK, BANDS, 1, LANES), jnp.float32), front_shape],
        input_output_aliases={0: 1},
        scratch_shapes=[pltpu.SemaphoreType.DMA],
        compiler_params=pltpu.CompilerParams(vmem_limit_bytes=2 << 20),
    )(front, g, pt)
    return out.reshape(8, BLK, 2, CHIPS, LANES).transpose(0, 1, 3, 2, 4).reshape(8, BLK, CHIPS, BLK)


def solution(mesh):
    in_specs = (
        P(None, "row", None, "col"),
        P("row", None, None),
        P("row", None, None),
        P(),
        P(),
        P(),
    )
    out_specs = P(None, "row", None, "col")
    return jax.shard_map(shards, mesh=mesh, in_specs=in_specs, out_specs=out_specs, check_vma=False)
```

```python
import math

import jax
import jax.numpy as jnp
from jax import lax
from jax.experimental import pallas as pl
from jax.experimental.pallas import tpu as pltpu
from jax.sharding import PartitionSpec as P

MESH = pl.DeviceIdType.MESH
CHIPS = 4
CORES = 2
SIDE = 4
GROUP = 12
WINDOW = 16
STRIPS = 16
BLK = 256
STRIP = BLK // STRIPS
LANES = 128
HALF = BLK // 2
BANDS = 8


def arrival_groups():
    names = ["S", "SF", "PR", "P0", "N0", "Q0", "CL", "CO", "CF", "DX", "DD"]
    for m in range(2):
        names += [("A1", m), ("A2", m), ("B1", m, 0), ("B1", m, 1), ("B1", m, 2), ("B2", m), ("A1r", m), ("B1r", m)]
    return {name: i for i, name in enumerate(names)}


GROUPS = arrival_groups()


def product(left, pt, b):
    tile = jnp.dot(left[0], pt[b, 0], preferred_element_type=jnp.float32)
    return tile + jnp.dot(left[1], pt[b, 1], preferred_element_type=jnp.float32)


def add_block(front, a, first, rows, b, tile):
    at = pl.ds(first, rows)
    for side in range(2):
        band = side * CHIPS + b
        front[a, band, at] = front[a, band, at] + tile[:, side * LANES:(side + 1) * LANES]


def quarter_rows(g, m, first):
    return [g[m, pl.ds(first, SIDE), 1:CHIPS, child].reshape(3 * SIDE * STRIP, BLK) for child in range(2)]


def add_quarter(front, y, m, first, b, tile):
    for n in range(SIDE):
        for d in (1, 2, 3):
            at = (n * 3 + d - 1) * STRIP
            add_block(front, 2 * ((y + d) % CHIPS) + m, (first + n) * STRIP, STRIP, b, tile[at:at + STRIP])


def gather_kernel(
    maps, counts, gen, diag, coup, parent, front, g, pt,
    bmap, vrows, cd, gp, gv, dv, cw, sb, sf, pb, dm, dx, dc, dd, lsem, ssem, dsem, rsem
):
    r = lax.axis_index("row")
    t = lax.axis_index("col")
    y, c = r // CORES, r % CORES
    z, x = t // SIDE, t % SIDE
    other = 1 - c
    partner = (y * CORES + other, t)
    pos = [(x, z), (z, x)]

    def wrap(v):
        return (v + 8) % 4

    def ydev(step, core):
        return (wrap(y + step) * CORES + core, t)

    def dev(m, dp, dq):
        p, q = wrap(pos[m][0] + dp), wrap(pos[m][1] + dq)
        return (r, q * SIDE + p) if m == 0 else (r, p * SIDE + q)

    def strip(m, dp, dq):
        return wrap(pos[m][1] + dq) * SIDE + wrap(pos[m][0] + dp)

    barrier = pltpu.get_barrier_semaphore()
    peers = [ydev(s, k) for s in (2, 1, 3) for k in range(CORES)] + [partner]
    peers += [dev(m, s, 0) for s in (1, -1) for m in range(2)]
    for peer in peers:
        pl.semaphore_signal(barrier, inc=1, device_id=peer, device_id_type=MESH)

    own_strip = [strip(0, 0, 0), strip(1, 0, 0)]
    load_strips = [
        pltpu.make_async_copy(gen.at[:, pl.ds(own_strip[m] * STRIP, STRIP), :], gp.at[m], lsem.at[0])
        for m in range(2)
    ]
    load_tables = [pltpu.make_async_copy(maps, bmap, lsem.at[1]), pltpu.make_async_copy(counts, vrows, lsem.at[2])]
    load_gen = pltpu.make_async_copy(gen, gv, lsem.at[3])
    load_diag = pltpu.make_async_copy(diag, dv, lsem.at[4])
    load_coup = pltpu.make_async_copy(coup, cw, lsem.at[5])
    load_front = [
        pltpu.make_async_copy(parent.at[a, :, band, 0, :], front.at[a, band], lsem.at[6])
        for a in range(8) for band in range(BANDS)
    ]
    for load in load_strips + load_tables + [load_gen, load_diag, load_coup]:
        load.start()
    zero = jnp.zeros((), jnp.bfloat16)
    down = lax.broadcasted_iota(jnp.int32, (BLK, BLK), 0)
    pltpu.make_async_copy(gp, gp, lsem.at[0]).wait()
    for load in load_tables:
        load.wait()

    entries = [bmap[c, y * GROUP + i] for i in range(GROUP)]

    def source(slot):
        at = y * WINDOW + slot
        before = jnp.int32(0)
        for e in entries:
            before = before + jnp.where(e < at, 1, 0).astype(jnp.int32)
        index = jnp.minimum(before, GROUP - 1)
        there = bmap[c, y * GROUP + index] == at
        return index, jnp.where(there, vrows[c, y * GROUP + index], 0)

    for m in range(2):
        for d in (2, 1, 3):
            for k in range(CORES):
                index, count = source(m * 8 + CORES * wrap(y - d) + k)
                inside = down[:STRIP] + own_strip[m] * STRIP < count
                sb[m, (d - 1) * CORES + k] = jnp.where(inside, gp[m, index], zero)

    pl.semaphore_wait(barrier, len(peers))

    sent = [0, 0]

    def send(group, src, dst, to):
        plane = int(isinstance(group, tuple))
        copy = pltpu.make_async_remote_copy(
            src_ref=src, dst_ref=dst, send_sem=ssem.at[plane], recv_sem=rsem.at[GROUPS[group]],
            device_id=to, device_id_type=MESH,
        )
        copy.start()
        sent[plane] += math.prod(src.shape)

    def arrived(group, size):
        pltpu.make_async_remote_copy(
            src_ref=size, dst_ref=size, send_sem=ssem.at[0], recv_sem=rsem.at[GROUPS[group]],
            device_id=partner, device_id_type=MESH,
        ).wait_recv()

    for d in (2, 1, 3):
        for m in range(2):
            for k in range(CORES):
                i = (d - 1) * CORES + k
                send("S", sb.at[m, i], g.at[m, own_strip[m], d, c], ydev(-d, k))
    load_gen.wait()
    index, wanted = source(t)
    cd[c, y] = jnp.where(down < wanted, gv[index], zero)
    for m in range(2):
        index, count = source(m * 8 + y * CORES + other)
        pb[m] = jnp.where(down < count, gv[index], zero).reshape(STRIPS, STRIP, BLK)

    def rows_of(k):
        return pl.ds(k * HALF, HALF)

    def onward(d):
        return 0 if d == 1 else 1

    for lead in (True, False):
        for d in (1, -1):
            half = cd.at[c, y, rows_of(onward(d) if lead else 1 - onward(d))]
            send("CL" if lead else "CO", half, half, ydev(d, c))
    send("P0", cd.at[c, y], cd.at[c, y], partner)
    far_strip = [strip(0, 2, 2), strip(1, 2, 2)]
    for m in range(2):
        send("PR", pb.at[m], g.at[m, :, 0, c], partner)
        index, count = source(m * 8 + r)
        g[m, :, 0, c] = jnp.where(down < count, gv[index], zero).reshape(STRIPS, STRIP, BLK)
        for d in (1, 2, 3):
            for k in range(CORES):
                index, count = source(m * 8 + CORES * wrap(y - d) + k)
                inside = down[:STRIP] + far_strip[m] * STRIP < count
                rows = gv[index, pl.ds(pl.multiple_of(far_strip[m] * STRIP, STRIP), STRIP)]
                sf[m, (d - 1) * CORES + k] = jnp.where(inside, rows, zero)
    load_diag.wait()
    across = lax.broadcasted_iota(jnp.int32, (BLK, BLK), 1)
    index, count = source(t)
    dm[...] = jnp.where(jnp.logical_and(down < count, across < count), dv[index], zero)
    for load in load_front:
        load.start()
    send("DX", dm.at[pl.ds(other * HALF, HALF)], dx, partner)
    load_coup.wait()
    for child in range(2):
        cw[child] = cw[child].T

    def piece(m, dp, dq, part=None):
        at = strip(m, dp, dq)
        if part is None:
            return g.at[m, at, pl.ds(1, 3)]
        return g.at[m, at, pl.ds(1, 3), part]

    def first_q(m, item):
        for d in (1, -1):
            ref = piece(m, item, 0)
            send(("B1", m, abs(item)), ref, ref, dev(m, 0, d))

    def second_q(m, items):
        arrived(("B1", m, abs(items[0])), g.at[m, pl.ds(0, 2), pl.ds(1, 3)])
        for item in items:
            for d in (1, -1):
                ref = piece(m, item, -d, onward(d))
                send(("B2", m), ref, ref, dev(m, 0, d))

    one_block = cd.at[0, 0]

    def project(s):
        for child in range(2):
            proj = lax.dot_general(
                cw[child], cd[child, s], (((1,), (1,)), ((), ())), preferred_element_type=jnp.float32
            )
            pt[s, child] = proj.astype(jnp.bfloat16)

    def add_to(a, first, rows, b, tile):
        add_block(front, a, first, rows, b, tile)

    def multiply(left, b):
        return product(left, pt, b)

    def own_tiles(b):
        for m in range(2):
            left = [g[m, :, 0, child].reshape(BLK, BLK) for child in range(2)]
            add_to(2 * y + m, 0, BLK, b, multiply(left, b))

    def quarter(m, dq):
        first = SIDE * wrap(z * (1 - m) + x * m + dq)
        left = quarter_rows(g, m, first)
        for b in range(CHIPS):
            add_quarter(front, y, m, first, b, multiply(left, b))

    arrived("P0", one_block)
    project(y)
    arrived("DX", dx)
    total = dm[pl.ds(c * HALF, HALF)].astype(jnp.float32) + dx[...].astype(jnp.float32)
    dc[...] = total.astype(jnp.bfloat16)
    arrived("PR", g.at[:, :, 0, 0])

    def diagonal_send():
        return pltpu.make_async_remote_copy(
            src_ref=dc, dst_ref=dd.at[y, pl.ds(c * HALF, HALF)], send_sem=dsem, recv_sem=rsem.at[GROUPS["DD"]],
            device_id=(t % 8, t), device_id_type=MESH,
        )

    arrived("S", g.at[0, pl.ds(0, 2), pl.ds(1, 3)])
    for lead in (True, False):
        for m in range(2):
            for d in (1, -1):
                ref = piece(m, 0, 0, onward(d) if lead else 1 - onward(d))
                send(("A1" if lead else "A1r", m), ref, ref, dev(m, d, 0))
    for m in range(2):
        first_q(m, 0)
    arrived("CL", one_block)
    for d in (1, -1):
        half = cd.at[c, wrap(y - d), rows_of(onward(d))]
        send("CF", half, half, ydev(d, c))
    for d in (2, 1, 3):
        for m in range(2):
            for k in range(CORES):
                send("SF", sf.at[m, (d - 1) * CORES + k], g.at[m, far_strip[m], d, c], ydev(-d, k))

    @pl.when(r != t % 8)
    def _():
        diagonal_send().start()

    pltpu.make_async_copy(front, front, lsem.at[6]).wait()
    own_tiles(y)
    arrived("CO", one_block)
    for d in (1, -1):
        ref = cd.at[c, wrap(y - d)]
        send("N0", ref, ref, partner)
    for m in range(2):
        arrived(("A1", m), g.at[m, 0, pl.ds(1, 3)])
        for d in (1, -1):
            ref = piece(m, -d, 0, onward(d))
            send(("A2", m), ref, ref, dev(m, d, 0))
    for m in range(2):
        for d in (1, -1):
            ref = piece(m, -d, 0, onward(d))
            send(("B1", m, 1), ref, ref, dev(m, 0, d))
    for m in range(2):
        arrived(("A1r", m), g.at[m, 0, pl.ds(1, 3)])
        for d in (1, -1):
            ref = piece(m, d, 0, onward(d))
            send(("B1", m, 1), ref, ref, dev(m, 0, d))
    for m in range(2):
        for d in (1, -1):
            for item in (1, -1):
                ref = piece(m, item, 0, 1 - onward(d))
                send(("B1r", m), ref, ref, dev(m, 0, d))
    for m in range(2):
        second_q(m, (0,))
    arrived("N0", cd.at[0, pl.ds(0, 2)])

    @pl.loop(0, 2)
    def _(i):
        project(wrap(y + 2 * i - 1))

    for m in range(2):
        arrived(("A2", m), g.at[m, 0, pl.ds(1, 3)])
        first_q(m, 2)
    arrived("CF", one_block)
    for d in (1, -1):
        half = cd.at[c, wrap(y + 2), rows_of(onward(d))]
        send("Q0", half, half, partner)

    for m in range(2):
        second_q(m, (1, -1))

    @pl.loop(0, 2)
    def _(i):
        own_tiles(wrap(y + 2 * i - 1))

    arrived("Q0", one_block)
    project(wrap(y + 2))
    own_tiles(wrap(y + 2))

    @pl.loop(0, 2)
    def _(m):
        quarter(m, 0)

    @pl.when(r == t % 8)
    def _():
        dd[y, pl.ds(c * HALF, HALF)] = dc[...]
        arrived("DD", gv.at[pl.ds(0, 7), pl.ds(0, HALF)])
        for b in range(CHIPS):
            add_to(2 * b + t // 8, 0, BLK, b, dd[b].astype(jnp.float32))

    @pl.when(r != t % 8)
    def _():
        diagonal_send().wait_send()

    for m in range(2):
        arrived(("B1r", m), g.at[m, pl.ds(0, 2), pl.ds(1, 3)])
        arrived(("B1", m, 2), g.at[m, pl.ds(0, 2), pl.ds(1, 3)])
    arrived("SF", g.at[0, pl.ds(0, 2), pl.ds(1, 3)])
    for m in range(2):
        arrived(("B2", m), g.at[m, pl.ds(0, 3), pl.ds(1, 3)])
    for plane in range(2):
        rows, rest = divmod(sent[plane], 2 * 2 * BANDS * LANES)
        assert rest == 0 and rows <= BLK and rows % 8 == 0
        size = front.at[pl.ds(0, 2), :, pl.ds(0, rows)]
        pltpu.make_async_remote_copy(
            src_ref=size, dst_ref=size, send_sem=ssem.at[plane], recv_sem=rsem.at[0],
            device_id=partner, device_id_type=MESH,
        ).wait_send()


def write_kernel(taken, g, pt, out, front, done):
    y = lax.axis_index("row") // CORES
    t = lax.axis_index("col")
    lines = [t // SIDE, t % SIDE]

    def write(a, b):
        for side in range(2):
            band = side * CHIPS + b
            pltpu.make_async_copy(front.at[a, band], out.at[a, :, band, 0, :], done).start()

    for m in range(2):
        for b in range(CHIPS):
            write(2 * y + m, b)
    for m in range(2):
        firsts = [SIDE * ((lines[m] + step) % SIDE) for step in (1, 3, 2)]
        lefts = [quarter_rows(g, m, first) for first in firsts]
        for b in range(CHIPS):
            for first, left in zip(firsts, lefts):
                add_quarter(front, y, m, first, b, product(left, pt, b))
            for d in (1, 2, 3):
                write(2 * ((y + d) % CHIPS) + m, b)
    pltpu.make_async_copy(front, front, done).wait()


def shards(parent_front, generators, diagonal_blocks, coupling, block_map, valid_rows):
    banded = parent_front.reshape(8, BLK, CHIPS, 2, LANES).transpose(0, 1, 3, 2, 4).reshape(8, BLK, BANDS, 1, LANES)
    any_spec = pl.BlockSpec(memory_space=pl.ANY)
    vmem = pl.BlockSpec(memory_space=pltpu.VMEM)
    bf16 = jnp.bfloat16
    front_shape = pltpu.VMEM((8, BANDS, BLK, LANES), jnp.float32)
    front, g, pt = pl.pallas_call(
        gather_kernel,
        name="gather",
        in_specs=[any_spec] * 6,
        out_specs=[vmem] * 3,
        out_shape=[
            front_shape,
            pltpu.VMEM((2, STRIPS, CHIPS, 2, STRIP, BLK), bf16),
            pltpu.VMEM((CHIPS, 2, BLK, BLK), bf16),
        ],
        scratch_shapes=[
            pltpu.SMEM(block_map.shape, jnp.int32),
            pltpu.SMEM(valid_rows.shape, jnp.int32),
            pltpu.VMEM((2, CHIPS, BLK, BLK), bf16),
            pltpu.VMEM((2, GROUP, STRIP, BLK), bf16),
            pltpu.VMEM((GROUP, BLK, BLK), bf16),
            pltpu.VMEM((GROUP, BLK, BLK), bf16),
            pltpu.VMEM((2, BLK, BLK), bf16),
            pltpu.VMEM((2, 6, STRIP, BLK), bf16),
            pltpu.VMEM((2, 6, STRIP, BLK), bf16),
            pltpu.VMEM((2, STRIPS, STRIP, BLK), bf16),
            pltpu.VMEM((BLK, BLK), bf16),
            pltpu.VMEM((HALF, BLK), bf16),
            pltpu.VMEM((HALF, BLK), bf16),
            pltpu.VMEM((CHIPS, BLK, BLK), bf16),
            pltpu.SemaphoreType.DMA((7,)),
            pltpu.SemaphoreType.DMA((2,)),
            pltpu.SemaphoreType.DMA,
            pltpu.SemaphoreType.DMA((len(GROUPS),)),
        ],
        compiler_params=pltpu.CompilerParams(
            collective_id=0, has_side_effects=True, vmem_limit_bytes=52 << 20
        ),
    )(block_map, valid_rows, generators, diagonal_blocks, coupling, banded)
    out, _ = pl.pallas_call(
        write_kernel,
        name="write",
        in_specs=[vmem] * 3,
        out_specs=[any_spec, vmem],
        out_shape=[jax.ShapeDtypeStruct((8, BLK, BANDS, 1, LANES), jnp.float32), front_shape],
        input_output_aliases={0: 1},
        scratch_shapes=[pltpu.SemaphoreType.DMA],
        compiler_params=pltpu.CompilerParams(vmem_limit_bytes=2 << 20),
    )(front, g, pt)
    return out.reshape(8, BLK, 2, CHIPS, LANES).transpose(0, 1, 3, 2, 4).reshape(8, BLK, CHIPS, BLK)


def solution(mesh):
    in_specs = (
        P(None, "row", None, "col"),
        P("row", None, None),
        P("row", None, None),
        P(),
        P(),
        P(),
    )
    out_specs = P(None, "row", None, "col")
    return jax.shard_map(shards, mesh=mesh, in_specs=in_specs, out_specs=out_specs, check_vma=False)
```

```python
import math

import jax
import jax.numpy as jnp
from jax import lax
from jax.experimental import pallas as pl
from jax.experimental.pallas import tpu as pltpu
from jax.sharding import PartitionSpec as P

MESH = pl.DeviceIdType.MESH
CHIPS = 4
CORES = 2
SIDE = 4
GROUP = 12
WINDOW = 16
STRIPS = 16
BLK = 256
STRIP = BLK // STRIPS
LANES = 128
HALF = BLK // 2
BANDS = 8


def arrival_groups():
    names = ["S", "end", "PR", "P0", "N0", "Q0", "CL", "CO", "CF", "DX", "DD"]
    for m in range(2):
        names += [("A1", m), ("A2", m), ("B1", m, 0), ("B1", m, 1), ("A1r", m)]
    return {name: i for i, name in enumerate(names)}


GROUPS = arrival_groups()


def product(left, pt, b):
    tile = jnp.dot(left[0], pt[b, 0], preferred_element_type=jnp.float32)
    return tile + jnp.dot(left[1], pt[b, 1], preferred_element_type=jnp.float32)


def add_block(front, a, first, rows, b, tile):
    at = pl.ds(first, rows)
    for side in range(2):
        band = side * CHIPS + b
        front[a, band, at] = front[a, band, at] + tile[:, side * LANES:(side + 1) * LANES]


def quarter_rows(g, m, first):
    return [g[m, pl.ds(first, SIDE), 1:CHIPS, child].reshape(3 * SIDE * STRIP, BLK) for child in range(2)]


def add_quarter(front, y, m, first, b, tile):
    for n in range(SIDE):
        for d in (1, 2, 3):
            at = (n * 3 + d - 1) * STRIP
            add_block(front, 2 * ((y + d) % CHIPS) + m, (first + n) * STRIP, STRIP, b, tile[at:at + STRIP])


def gather_kernel(
    maps, counts, gen, diag, coup, parent, front, g, pt,
    bmap, vrows, cd, gp, gv, dv, cw, sb, sf, pb, dm, dx, dc, dd, lsem, ssem, dsem, rsem
):
    r = lax.axis_index("row")
    t = lax.axis_index("col")
    y, c = r // CORES, r % CORES
    z, x = t // SIDE, t % SIDE
    other = 1 - c
    partner = (y * CORES + other, t)
    pos = [(x, z), (z, x)]

    def wrap(v):
        return (v + 8) % 4

    def ydev(step, core):
        return (wrap(y + step) * CORES + core, t)

    def dev(m, dp, dq):
        p, q = wrap(pos[m][0] + dp), wrap(pos[m][1] + dq)
        return (r, q * SIDE + p) if m == 0 else (r, p * SIDE + q)

    def strip(m, dp, dq):
        return wrap(pos[m][1] + dq) * SIDE + wrap(pos[m][0] + dp)

    barrier = pltpu.get_barrier_semaphore()
    peers = [ydev(s, k) for s in (2, 1, 3) for k in range(CORES)] + [partner]
    peers += [dev(m, s, 0) for s in (1, -1) for m in range(2)]
    for peer in peers:
        pl.semaphore_signal(barrier, inc=1, device_id=peer, device_id_type=MESH)

    own_strip = [strip(0, 0, 0), strip(1, 0, 0)]
    load_strips = [
        pltpu.make_async_copy(gen.at[:, pl.ds(own_strip[m] * STRIP, STRIP), :], gp.at[m], lsem.at[0])
        for m in range(2)
    ]
    load_tables = [pltpu.make_async_copy(maps, bmap, lsem.at[1]), pltpu.make_async_copy(counts, vrows, lsem.at[2])]
    load_gen = pltpu.make_async_copy(gen, gv, lsem.at[3])
    load_diag = pltpu.make_async_copy(diag, dv, lsem.at[4])
    load_coup = pltpu.make_async_copy(coup, cw, lsem.at[5])
    load_front = [
        pltpu.make_async_copy(parent.at[a, :, band, 0, :], front.at[a, band], lsem.at[6])
        for a in range(8) for band in range(BANDS)
    ]
    for load in load_strips + load_tables + [load_gen, load_diag, load_coup]:
        load.start()
    zero = jnp.zeros((), jnp.bfloat16)
    down = lax.broadcasted_iota(jnp.int32, (BLK, BLK), 0)
    pltpu.make_async_copy(gp, gp, lsem.at[0]).wait()
    for load in load_tables:
        load.wait()

    entries = [bmap[c, y * GROUP + i] for i in range(GROUP)]

    def source(slot):
        at = y * WINDOW + slot
        before = jnp.int32(0)
        for e in entries:
            before = before + jnp.where(e < at, 1, 0).astype(jnp.int32)
        index = jnp.minimum(before, GROUP - 1)
        there = bmap[c, y * GROUP + index] == at
        return index, jnp.where(there, vrows[c, y * GROUP + index], 0)

    for m in range(2):
        for d in (2, 1, 3):
            for k in range(CORES):
                index, count = source(m * 8 + CORES * wrap(y - d) + k)
                inside = down[:STRIP] + own_strip[m] * STRIP < count
                sb[m, (d - 1) * CORES + k] = jnp.where(inside, gp[m, index], zero)

    pl.semaphore_wait(barrier, len(peers))

    sent = [0, 0]

    def send(group, src, dst, to):
        plane = int(to[0] is r)
        copy = pltpu.make_async_remote_copy(
            src_ref=src, dst_ref=dst, send_sem=ssem.at[plane], recv_sem=rsem.at[GROUPS[group]],
            device_id=to, device_id_type=MESH,
        )
        copy.start()
        sent[plane] += math.prod(src.shape)

    def arrived(group, size):
        pltpu.make_async_remote_copy(
            src_ref=size, dst_ref=size, send_sem=ssem.at[0], recv_sem=rsem.at[GROUPS[group]],
            device_id=partner, device_id_type=MESH,
        ).wait_recv()

    for d in (2, 1, 3):
        for m in range(2):
            for k in range(CORES):
                i = (d - 1) * CORES + k
                send("S", sb.at[m, i], g.at[m, own_strip[m], d, c], ydev(-d, k))
    load_gen.wait()
    index, wanted = source(t)
    cd[c, y] = jnp.where(down < wanted, gv[index], zero)
    for m in range(2):
        index, count = source(m * 8 + y * CORES + other)
        pb[m] = jnp.where(down < count, gv[index], zero).reshape(STRIPS, STRIP, BLK)

    def rows_of(k):
        return pl.ds(k * HALF, HALF)

    def onward(d):
        return 0 if d == 1 else 1

    for lead in (True, False):
        for d in (1, -1):
            half = cd.at[c, y, rows_of(onward(d) if lead else 1 - onward(d))]
            send("CL" if lead else "CO", half, half, ydev(d, c))
    send("P0", cd.at[c, y], cd.at[c, y], partner)
    far_strip = [strip(0, 2, 2), strip(1, 2, 2)]
    for m in range(2):
        send("PR", pb.at[m], g.at[m, :, 0, c], partner)
        index, count = source(m * 8 + r)
        g[m, :, 0, c] = jnp.where(down < count, gv[index], zero).reshape(STRIPS, STRIP, BLK)
        for d in (1, 2, 3):
            for k in range(CORES):
                index, count = source(m * 8 + CORES * wrap(y - d) + k)
                inside = down[:STRIP] + far_strip[m] * STRIP < count
                rows = gv[index, pl.ds(pl.multiple_of(far_strip[m] * STRIP, STRIP), STRIP)]
                sf[m, (d - 1) * CORES + k] = jnp.where(inside, rows, zero)
    load_diag.wait()
    across = lax.broadcasted_iota(jnp.int32, (BLK, BLK), 1)
    index, count = source(t)
    dm[...] = jnp.where(jnp.logical_and(down < count, across < count), dv[index], zero)
    for load in load_front:
        load.start()
    send("DX", dm.at[pl.ds(other * HALF, HALF)], dx, partner)
    load_coup.wait()
    for child in range(2):
        cw[child] = cw[child].T

    def piece(m, dp, dq, part=None):
        at = strip(m, dp, dq)
        if part is None:
            return g.at[m, at, pl.ds(1, 3)]
        return g.at[m, at, pl.ds(1, 3), part]

    def first_q(m, item, child, group, d):
        ref = piece(m, item, 0, child)
        send(group, ref, ref, dev(m, 0, d))

    def second_q(m, items):
        arrived(("B1", m, abs(items[0])), g.at[m, pl.ds(0, len(items)), pl.ds(1, 3)])
        for item in items:
            for d in (1, -1):
                ref = piece(m, item, -d, onward(d))
                send("end", ref, ref, dev(m, 0, d))

    one_block = cd.at[0, 0]

    def project(s):
        for child in range(2):
            proj = lax.dot_general(
                cw[child], cd[child, s], (((1,), (1,)), ((), ())), preferred_element_type=jnp.float32
            )
            pt[s, child] = proj.astype(jnp.bfloat16)

    def add_to(a, first, rows, b, tile):
        add_block(front, a, first, rows, b, tile)

    def multiply(left, b):
        return product(left, pt, b)

    def own_tiles(b):
        for m in range(2):
            left = [g[m, :, 0, child].reshape(BLK, BLK) for child in range(2)]
            add_to(2 * y + m, 0, BLK, b, multiply(left, b))

    def quarter(m, dq):
        first = SIDE * wrap(z * (1 - m) + x * m + dq)
        left = quarter_rows(g, m, first)
        for b in range(CHIPS):
            add_quarter(front, y, m, first, b, multiply(left, b))

    arrived("P0", one_block)
    project(y)
    arrived("DX", dx)
    total = dm[pl.ds(c * HALF, HALF)].astype(jnp.float32) + dx[...].astype(jnp.float32)
    dc[...] = total.astype(jnp.bfloat16)
    arrived("PR", g.at[:, :, 0, 0])

    def diagonal_send():
        return pltpu.make_async_remote_copy(
            src_ref=dc, dst_ref=dd.at[y, pl.ds(c * HALF, HALF)], send_sem=dsem, recv_sem=rsem.at[GROUPS["DD"]],
            device_id=(t % 8, t), device_id_type=MESH,
        )

    arrived("S", g.at[0, pl.ds(0, 2), pl.ds(1, 3)])
    for lead in (True, False):
        for m in range(2):
            for d in (1, -1):
                ref = piece(m, 0, 0, onward(d) if lead else 1 - onward(d))
                send(("A1" if lead else "A1r", m), ref, ref, dev(m, d, 0))
    for m in range(2):
        for d in (1, -1):
            first_q(m, 0, onward(d), ("B1", m, 0), d)
    for m in range(2):
        for d in (1, -1):
            first_q(m, 0, 1 - onward(d), "end", d)
    arrived("CL", one_block)
    for d in (1, -1):
        half = cd.at[c, wrap(y - d), rows_of(onward(d))]
        send("CF", half, half, ydev(d, c))
    for d in (2, 1, 3):
        for m in range(2):
            for k in range(CORES):
                send("end", sf.at[m, (d - 1) * CORES + k], g.at[m, far_strip[m], d, c], ydev(-d, k))

    @pl.when(r != t % 8)
    def _():
        diagonal_send().start()

    pltpu.make_async_copy(front, front, lsem.at[6]).wait()
    own_tiles(y)
    for m in range(2):
        arrived(("A1", m), g.at[m, 0, pl.ds(1, 3)])
        for d in (1, -1):
            ref = piece(m, -d, 0, onward(d))
            send(("A2", m), ref, ref, dev(m, d, 0))
    for m in range(2):
        for d in (1, -1):
            ref = piece(m, -d, 0, onward(d))
            send(("B1", m, 1), ref, ref, dev(m, 0, d))
    for m in range(2):
        arrived(("A1r", m), g.at[m, 0, pl.ds(1, 3)])
        for d in (1, -1):
            ref = piece(m, d, 0, onward(d))
            send(("B1", m, 1), ref, ref, dev(m, 0, d))
    for m in range(2):
        for d in (1, -1):
            for item in (1, -1):
                ref = piece(m, item, 0, 1 - onward(d))
                send("end", ref, ref, dev(m, 0, d))
    arrived("CO", one_block)
    for d in (1, -1):
        ref = cd.at[c, wrap(y - d)]
        send("N0", ref, ref, partner)
    for m in range(2):
        second_q(m, (0,))
    arrived("N0", cd.at[0, pl.ds(0, 2)])

    @pl.loop(0, 2)
    def _(i):
        project(wrap(y + 2 * i - 1))

    for m in range(2):
        arrived(("A2", m), g.at[m, 0, pl.ds(1, 3)])
        for d in (1, -1):
            first_q(m, 2, None, "end", d)
    arrived("CF", one_block)
    for d in (1, -1):
        half = cd.at[c, wrap(y + 2), rows_of(onward(d))]
        send("Q0", half, half, partner)

    for m in range(2):
        second_q(m, (1, -1))

    @pl.loop(0, 2)
    def _(i):
        own_tiles(wrap(y + 2 * i - 1))

    arrived("Q0", one_block)
    project(wrap(y + 2))
    own_tiles(wrap(y + 2))

    @pl.loop(0, 2)
    def _(m):
        quarter(m, 0)

    @pl.when(r == t % 8)
    def _():
        dd[y, pl.ds(c * HALF, HALF)] = dc[...]
        arrived("DD", gv.at[pl.ds(0, 7), pl.ds(0, HALF)])
        for b in range(CHIPS):
            add_to(2 * b + t // 8, 0, BLK, b, dd[b].astype(jnp.float32))

    @pl.when(r != t % 8)
    def _():
        diagonal_send().wait_send()

    arrived("end", g.at[:, pl.ds(0, 9), pl.ds(1, 3)])
    for plane in range(2):
        rows, rest = divmod(sent[plane], 2 * 2 * BANDS * LANES)
        assert rest == 0 and rows <= BLK and rows % 8 == 0
        size = front.at[pl.ds(0, 2), :, pl.ds(0, rows)]
        pltpu.make_async_remote_copy(
            src_ref=size, dst_ref=size, send_sem=ssem.at[plane], recv_sem=rsem.at[0],
            device_id=partner, device_id_type=MESH,
        ).wait_send()


def write_kernel(taken, g, pt, out, front, done):
    y = lax.axis_index("row") // CORES
    t = lax.axis_index("col")
    lines = [t // SIDE, t % SIDE]

    def write(a, b):
        for side in range(2):
            band = side * CHIPS + b
            pltpu.make_async_copy(front.at[a, band], out.at[a, :, band, 0, :], done).start()

    for m in range(2):
        for b in range(CHIPS):
            write(2 * y + m, b)
    for m in range(2):
        firsts = [SIDE * ((lines[m] + step) % SIDE) for step in (1, 3, 2)]
        lefts = [quarter_rows(g, m, first) for first in firsts]
        for b in range(CHIPS):
            for first, left in zip(firsts, lefts):
                add_quarter(front, y, m, first, b, product(left, pt, b))
            for d in (1, 2, 3):
                write(2 * ((y + d) % CHIPS) + m, b)
    pltpu.make_async_copy(front, front, done).wait()


def shards(parent_front, generators, diagonal_blocks, coupling, block_map, valid_rows):
    banded = parent_front.reshape(8, BLK, CHIPS, 2, LANES).transpose(0, 1, 3, 2, 4).reshape(8, BLK, BANDS, 1, LANES)
    any_spec = pl.BlockSpec(memory_space=pl.ANY)
    vmem = pl.BlockSpec(memory_space=pltpu.VMEM)
    bf16 = jnp.bfloat16
    front_shape = pltpu.VMEM((8, BANDS, BLK, LANES), jnp.float32)
    front, g, pt = pl.pallas_call(
        gather_kernel,
        name="gather",
        in_specs=[any_spec] * 6,
        out_specs=[vmem] * 3,
        out_shape=[
            front_shape,
            pltpu.VMEM((2, STRIPS, CHIPS, 2, STRIP, BLK), bf16),
            pltpu.VMEM((CHIPS, 2, BLK, BLK), bf16),
        ],
        scratch_shapes=[
            pltpu.SMEM(block_map.shape, jnp.int32),
            pltpu.SMEM(valid_rows.shape, jnp.int32),
            pltpu.VMEM((2, CHIPS, BLK, BLK), bf16),
            pltpu.VMEM((2, GROUP, STRIP, BLK), bf16),
            pltpu.VMEM((GROUP, BLK, BLK), bf16),
            pltpu.VMEM((GROUP, BLK, BLK), bf16),
            pltpu.VMEM((2, BLK, BLK), bf16),
            pltpu.VMEM((2, 6, STRIP, BLK), bf16),
            pltpu.VMEM((2, 6, STRIP, BLK), bf16),
            pltpu.VMEM((2, STRIPS, STRIP, BLK), bf16),
            pltpu.VMEM((BLK, BLK), bf16),
            pltpu.VMEM((HALF, BLK), bf16),
            pltpu.VMEM((HALF, BLK), bf16),
            pltpu.VMEM((CHIPS, BLK, BLK), bf16),
            pltpu.SemaphoreType.DMA((7,)),
            pltpu.SemaphoreType.DMA((2,)),
            pltpu.SemaphoreType.DMA,
            pltpu.SemaphoreType.DMA((len(GROUPS),)),
        ],
        compiler_params=pltpu.CompilerParams(
            collective_id=0, has_side_effects=True, vmem_limit_bytes=52 << 20
        ),
    )(block_map, valid_rows, generators, diagonal_blocks, coupling, banded)
    out, _ = pl.pallas_call(
        write_kernel,
        name="write",
        in_specs=[vmem] * 3,
        out_specs=[any_spec, vmem],
        out_shape=[jax.ShapeDtypeStruct((8, BLK, BANDS, 1, LANES), jnp.float32), front_shape],
        input_output_aliases={0: 1},
        scratch_shapes=[pltpu.SemaphoreType.DMA],
        compiler_params=pltpu.CompilerParams(vmem_limit_bytes=2 << 20),
    )(front, g, pt)
    return out.reshape(8, BLK, 2, CHIPS, LANES).transpose(0, 1, 3, 2, 4).reshape(8, BLK, CHIPS, BLK)


def solution(mesh):
    in_specs = (
        P(None, "row", None, "col"),
        P("row", None, None),
        P("row", None, None),
        P(),
        P(),
        P(),
    )
    out_specs = P(None, "row", None, "col")
    return jax.shard_map(shards, mesh=mesh, in_specs=in_specs, out_specs=out_specs, check_vma=False)
```

```python
import math

import jax
import jax.numpy as jnp
from jax import lax
from jax.experimental import pallas as pl
from jax.experimental.pallas import tpu as pltpu
from jax.sharding import PartitionSpec as P

MESH = pl.DeviceIdType.MESH
CHIPS = 4
CORES = 2
SIDE = 4
GROUP = 12
WINDOW = 16
STRIPS = 16
BLK = 256
STRIP = BLK // STRIPS
LANES = 128
HALF = BLK // 2
BANDS = 8


def arrival_groups():
    names = ["S", "end", "PR", "P0", "N0", "Q0", "CL", "CO", "CF", "DX", "DD"]
    for m in range(2):
        names += [("A1", m), ("A2", m), ("B1", m, 0), ("B1", m, 1), ("A1r", m)]
    return {name: i for i, name in enumerate(names)}


GROUPS = arrival_groups()


def product(left, pt, b):
    tile = jnp.dot(left[0], pt[b, 0], preferred_element_type=jnp.float32)
    return tile + jnp.dot(left[1], pt[b, 1], preferred_element_type=jnp.float32)


def add_block(front, a, first, rows, b, tile):
    at = pl.ds(first, rows)
    for side in range(2):
        band = side * CHIPS + b
        front[a, band, at] = front[a, band, at] + tile[:, side * LANES:(side + 1) * LANES]


def quarter_rows(g, m, first):
    return [g[m, pl.ds(first, SIDE), 1:CHIPS, child].reshape(3 * SIDE * STRIP, BLK) for child in range(2)]


def add_quarter(front, y, m, first, b, tile):
    for n in range(SIDE):
        for d in (1, 2, 3):
            at = (n * 3 + d - 1) * STRIP
            add_block(front, 2 * ((y + d) % CHIPS) + m, (first + n) * STRIP, STRIP, b, tile[at:at + STRIP])


def gather_kernel(
    maps, counts, gen, diag, coup, parent, front, g, pt,
    bmap, vrows, cd, gp, gv, dv, cw, sb, sf, pb, dm, dx, dc, dd, lsem, ssem, dsem, rsem
):
    r = lax.axis_index("row")
    t = lax.axis_index("col")
    y, c = r // CORES, r % CORES
    z, x = t // SIDE, t % SIDE
    other = 1 - c
    partner = (y * CORES + other, t)
    pos = [(x, z), (z, x)]

    def wrap(v):
        return (v + 8) % 4

    def ydev(step, core):
        return (wrap(y + step) * CORES + core, t)

    def dev(m, dp, dq):
        p, q = wrap(pos[m][0] + dp), wrap(pos[m][1] + dq)
        return (r, q * SIDE + p) if m == 0 else (r, p * SIDE + q)

    def strip(m, dp, dq):
        return wrap(pos[m][1] + dq) * SIDE + wrap(pos[m][0] + dp)

    barrier = pltpu.get_barrier_semaphore()
    peers = [ydev(s, k) for s in (2, 1, 3) for k in range(CORES)] + [partner]
    peers += [dev(m, s, 0) for s in (1, -1) for m in range(2)]
    for peer in peers:
        pl.semaphore_signal(barrier, inc=1, device_id=peer, device_id_type=MESH)

    own_strip = [strip(0, 0, 0), strip(1, 0, 0)]
    load_strips = [
        pltpu.make_async_copy(gen.at[:, pl.ds(own_strip[m] * STRIP, STRIP), :], gp.at[m], lsem.at[0])
        for m in range(2)
    ]
    load_tables = [pltpu.make_async_copy(maps, bmap, lsem.at[1]), pltpu.make_async_copy(counts, vrows, lsem.at[2])]
    load_gen = pltpu.make_async_copy(gen, gv, lsem.at[3])
    load_diag = pltpu.make_async_copy(diag, dv, lsem.at[4])
    load_coup = pltpu.make_async_copy(coup, cw, lsem.at[5])
    load_front = [
        pltpu.make_async_copy(parent.at[a, :, band, 0, :], front.at[a, band], lsem.at[6])
        for a in range(8) for band in range(BANDS)
    ]
    for load in load_strips + load_tables + [load_gen, load_diag, load_coup]:
        load.start()
    zero = jnp.zeros((), jnp.bfloat16)
    down = lax.broadcasted_iota(jnp.int32, (BLK, BLK), 0)
    pltpu.make_async_copy(gp, gp, lsem.at[0]).wait()
    for load in load_tables:
        load.wait()

    entries = [bmap[c, y * GROUP + i] for i in range(GROUP)]

    def source(slot):
        at = y * WINDOW + slot
        before = jnp.int32(0)
        for e in entries:
            before = before + jnp.where(e < at, 1, 0).astype(jnp.int32)
        index = jnp.minimum(before, GROUP - 1)
        there = bmap[c, y * GROUP + index] == at
        return index, jnp.where(there, vrows[c, y * GROUP + index], 0)

    for m in range(2):
        for d in (2, 1, 3):
            for k in range(CORES):
                index, count = source(m * 8 + CORES * wrap(y - d) + k)
                inside = down[:STRIP] + own_strip[m] * STRIP < count
                sb[m, (d - 1) * CORES + k] = jnp.where(inside, gp[m, index], zero)

    pl.semaphore_wait(barrier, len(peers))

    sent = [0, 0]

    def send(group, src, dst, to):
        plane = int(to[0] is r)
        copy = pltpu.make_async_remote_copy(
            src_ref=src, dst_ref=dst, send_sem=ssem.at[plane], recv_sem=rsem.at[GROUPS[group]],
            device_id=to, device_id_type=MESH,
        )
        copy.start()
        sent[plane] += math.prod(src.shape)

    def arrived(group, size):
        pltpu.make_async_remote_copy(
            src_ref=size, dst_ref=size, send_sem=ssem.at[0], recv_sem=rsem.at[GROUPS[group]],
            device_id=partner, device_id_type=MESH,
        ).wait_recv()

    for d in (2, 1, 3):
        for m in range(2):
            for k in range(CORES):
                i = (d - 1) * CORES + k
                send("S", sb.at[m, i], g.at[m, own_strip[m], d, c], ydev(-d, k))
    load_gen.wait()
    index, wanted = source(t)
    cd[c, y] = jnp.where(down < wanted, gv[index], zero)
    for m in range(2):
        index, count = source(m * 8 + y * CORES + other)
        pb[m] = jnp.where(down < count, gv[index], zero).reshape(STRIPS, STRIP, BLK)

    def rows_of(k):
        return pl.ds(k * HALF, HALF)

    def onward(d):
        return 0 if d == 1 else 1

    for lead in (True, False):
        for d in (1, -1):
            half = cd.at[c, y, rows_of(onward(d) if lead else 1 - onward(d))]
            send("CL" if lead else "CO", half, half, ydev(d, c))
    send("P0", cd.at[c, y], cd.at[c, y], partner)
    far_strip = [strip(0, 2, 2), strip(1, 2, 2)]
    for m in range(2):
        send("PR", pb.at[m], g.at[m, :, 0, c], partner)
        index, count = source(m * 8 + r)
        g[m, :, 0, c] = jnp.where(down < count, gv[index], zero).reshape(STRIPS, STRIP, BLK)
        for d in (1, 2, 3):
            for k in range(CORES):
                index, count = source(m * 8 + CORES * wrap(y - d) + k)
                inside = down[:STRIP] + far_strip[m] * STRIP < count
                rows = gv[index, pl.ds(pl.multiple_of(far_strip[m] * STRIP, STRIP), STRIP)]
                sf[m, (d - 1) * CORES + k] = jnp.where(inside, rows, zero)
    load_diag.wait()
    across = lax.broadcasted_iota(jnp.int32, (BLK, BLK), 1)
    index, count = source(t)
    dm[...] = jnp.where(jnp.logical_and(down < count, across < count), dv[index], zero)
    for load in load_front:
        load.start()
    send("DX", dm.at[pl.ds(other * HALF, HALF)], dx, partner)
    load_coup.wait()
    for child in range(2):
        cw[child] = cw[child].T

    def piece(m, dp, dq, part=None):
        at = strip(m, dp, dq)
        if part is None:
            return g.at[m, at, pl.ds(1, 3)]
        return g.at[m, at, pl.ds(1, 3), part]

    def first_q(m, item, child, group, d):
        ref = piece(m, item, 0, child)
        send(group, ref, ref, dev(m, 0, d))

    def second_q(m, items):
        arrived(("B1", m, abs(items[0])), g.at[m, pl.ds(0, len(items)), pl.ds(1, 3)])
        for item in items:
            for d in (1, -1):
                ref = piece(m, item, -d, onward(d))
                send("end", ref, ref, dev(m, 0, d))

    one_block = cd.at[0, 0]

    def project(s):
        for child in range(2):
            proj = lax.dot_general(
                cw[child], cd[child, s], (((1,), (1,)), ((), ())), preferred_element_type=jnp.float32
            )
            pt[s, child] = proj.astype(jnp.bfloat16)

    def add_to(a, first, rows, b, tile):
        add_block(front, a, first, rows, b, tile)

    def multiply(left, b):
        return product(left, pt, b)

    def own_tiles(b):
        for m in range(2):
            left = [g[m, :, 0, child].reshape(BLK, BLK) for child in range(2)]
            add_to(2 * y + m, 0, BLK, b, multiply(left, b))

    def quarter(m, dq):
        first = SIDE * wrap(z * (1 - m) + x * m + dq)
        left = quarter_rows(g, m, first)
        for b in range(CHIPS):
            add_quarter(front, y, m, first, b, multiply(left, b))

    arrived("P0", one_block)
    project(y)
    arrived("DX", dx)
    total = dm[pl.ds(c * HALF, HALF)].astype(jnp.float32) + dx[...].astype(jnp.float32)
    dc[...] = total.astype(jnp.bfloat16)
    arrived("PR", g.at[:, :, 0, 0])

    def diagonal_send():
        return pltpu.make_async_remote_copy(
            src_ref=dc, dst_ref=dd.at[y, pl.ds(c * HALF, HALF)], send_sem=dsem, recv_sem=rsem.at[GROUPS["DD"]],
            device_id=(t % 8, t), device_id_type=MESH,
        )

    arrived("S", g.at[0, pl.ds(0, 2), pl.ds(1, 3)])
    for lead in (True, False):
        for m in range(2):
            for d in (1, -1):
                ref = piece(m, 0, 0, onward(d) if lead else 1 - onward(d))
                send(("A1" if lead else "A1r", m), ref, ref, dev(m, d, 0))
    for m in range(2):
        for d in (1, -1):
            first_q(m, 0, onward(d), ("B1", m, 0), d)
    for m in range(2):
        for d in (1, -1):
            first_q(m, 0, 1 - onward(d), "end", d)
    arrived("CL", one_block)
    for d in (1, -1):
        half = cd.at[c, wrap(y - d), rows_of(onward(d))]
        send("CF", half, half, ydev(d, c))
    pltpu.make_async_copy(front, front, lsem.at[6]).wait()
    own_tiles(y)
    for m in range(2):
        arrived(("A1", m), g.at[m, 0, pl.ds(1, 3)])
        for d in (1, -1):
            ref = piece(m, -d, 0, onward(d))
            send(("A2", m), ref, ref, dev(m, d, 0))
    for m in range(2):
        for d in (1, -1):
            ref = piece(m, -d, 0, onward(d))
            send(("B1", m, 1), ref, ref, dev(m, 0, d))
    for m in range(2):
        arrived(("A1r", m), g.at[m, 0, pl.ds(1, 3)])
        for d in (1, -1):
            ref = piece(m, d, 0, onward(d))
            send(("B1", m, 1), ref, ref, dev(m, 0, d))
    for m in range(2):
        for d in (1, -1):
            for item in (1, -1):
                ref = piece(m, item, 0, 1 - onward(d))
                send("end", ref, ref, dev(m, 0, d))
    for d in (2, 1, 3):
        for m in range(2):
            for k in range(CORES):
                send("end", sf.at[m, (d - 1) * CORES + k], g.at[m, far_strip[m], d, c], ydev(-d, k))

    @pl.when(r != t % 8)
    def _():
        diagonal_send().start()

    arrived("CO", one_block)
    for d in (1, -1):
        ref = cd.at[c, wrap(y - d)]
        send("N0", ref, ref, partner)
    arrived("N0", cd.at[0, pl.ds(0, 2)])

    @pl.loop(0, 2)
    def _(i):
        project(wrap(y + 2 * i - 1))

    for m in range(2):
        second_q(m, (0,))
    for m in range(2):
        arrived(("A2", m), g.at[m, 0, pl.ds(1, 3)])
        for d in (1, -1):
            first_q(m, 2, None, "end", d)
    arrived("CF", one_block)
    for d in (1, -1):
        half = cd.at[c, wrap(y + 2), rows_of(onward(d))]
        send("Q0", half, half, partner)

    for m in range(2):
        second_q(m, (1, -1))

    @pl.loop(0, 2)
    def _(i):
        own_tiles(wrap(y + 2 * i - 1))

    arrived("Q0", one_block)
    project(wrap(y + 2))
    own_tiles(wrap(y + 2))

    @pl.loop(0, 2)
    def _(m):
        quarter(m, 0)

    @pl.when(r == t % 8)
    def _():
        dd[y, pl.ds(c * HALF, HALF)] = dc[...]
        arrived("DD", gv.at[pl.ds(0, 7), pl.ds(0, HALF)])
        for b in range(CHIPS):
            add_to(2 * b + t // 8, 0, BLK, b, dd[b].astype(jnp.float32))

    @pl.when(r != t % 8)
    def _():
        diagonal_send().wait_send()

    arrived("end", g.at[:, pl.ds(0, 9), pl.ds(1, 3)])
    for plane in range(2):
        rows, rest = divmod(sent[plane], 2 * 2 * BANDS * LANES)
        assert rest == 0 and rows <= BLK and rows % 8 == 0
        size = front.at[pl.ds(0, 2), :, pl.ds(0, rows)]
        pltpu.make_async_remote_copy(
            src_ref=size, dst_ref=size, send_sem=ssem.at[plane], recv_sem=rsem.at[0],
            device_id=partner, device_id_type=MESH,
        ).wait_send()


def write_kernel(taken, g, pt, out, front, done):
    y = lax.axis_index("row") // CORES
    t = lax.axis_index("col")
    lines = [t // SIDE, t % SIDE]

    def write(a, b):
        for side in range(2):
            band = side * CHIPS + b
            pltpu.make_async_copy(front.at[a, band], out.at[a, :, band, 0, :], done).start()

    for m in range(2):
        for b in range(CHIPS):
            write(2 * y + m, b)
    for m in range(2):
        firsts = [SIDE * ((lines[m] + step) % SIDE) for step in (1, 3, 2)]
        lefts = [quarter_rows(g, m, first) for first in firsts]
        for b in range(CHIPS):
            for first, left in zip(firsts, lefts):
                add_quarter(front, y, m, first, b, product(left, pt, b))
            for d in (1, 2, 3):
                write(2 * ((y + d) % CHIPS) + m, b)
    pltpu.make_async_copy(front, front, done).wait()


def shards(parent_front, generators, diagonal_blocks, coupling, block_map, valid_rows):
    banded = parent_front.reshape(8, BLK, CHIPS, 2, LANES).transpose(0, 1, 3, 2, 4).reshape(8, BLK, BANDS, 1, LANES)
    any_spec = pl.BlockSpec(memory_space=pl.ANY)
    vmem = pl.BlockSpec(memory_space=pltpu.VMEM)
    bf16 = jnp.bfloat16
    front_shape = pltpu.VMEM((8, BANDS, BLK, LANES), jnp.float32)
    front, g, pt = pl.pallas_call(
        gather_kernel,
        name="gather",
        in_specs=[any_spec] * 6,
        out_specs=[vmem] * 3,
        out_shape=[
            front_shape,
            pltpu.VMEM((2, STRIPS, CHIPS, 2, STRIP, BLK), bf16),
            pltpu.VMEM((CHIPS, 2, BLK, BLK), bf16),
        ],
        scratch_shapes=[
            pltpu.SMEM(block_map.shape, jnp.int32),
            pltpu.SMEM(valid_rows.shape, jnp.int32),
            pltpu.VMEM((2, CHIPS, BLK, BLK), bf16),
            pltpu.VMEM((2, GROUP, STRIP, BLK), bf16),
            pltpu.VMEM((GROUP, BLK, BLK), bf16),
            pltpu.VMEM((GROUP, BLK, BLK), bf16),
            pltpu.VMEM((2, BLK, BLK), bf16),
            pltpu.VMEM((2, 6, STRIP, BLK), bf16),
            pltpu.VMEM((2, 6, STRIP, BLK), bf16),
            pltpu.VMEM((2, STRIPS, STRIP, BLK), bf16),
            pltpu.VMEM((BLK, BLK), bf16),
            pltpu.VMEM((HALF, BLK), bf16),
            pltpu.VMEM((HALF, BLK), bf16),
            pltpu.VMEM((CHIPS, BLK, BLK), bf16),
            pltpu.SemaphoreType.DMA((7,)),
            pltpu.SemaphoreType.DMA((2,)),
            pltpu.SemaphoreType.DMA,
            pltpu.SemaphoreType.DMA((len(GROUPS),)),
        ],
        compiler_params=pltpu.CompilerParams(
            collective_id=0, has_side_effects=True, vmem_limit_bytes=52 << 20
        ),
    )(block_map, valid_rows, generators, diagonal_blocks, coupling, banded)
    out, _ = pl.pallas_call(
        write_kernel,
        name="write",
        in_specs=[vmem] * 3,
        out_specs=[any_spec, vmem],
        out_shape=[jax.ShapeDtypeStruct((8, BLK, BANDS, 1, LANES), jnp.float32), front_shape],
        input_output_aliases={0: 1},
        scratch_shapes=[pltpu.SemaphoreType.DMA],
        compiler_params=pltpu.CompilerParams(vmem_limit_bytes=2 << 20),
    )(front, g, pt)
    return out.reshape(8, BLK, 2, CHIPS, LANES).transpose(0, 1, 3, 2, 4).reshape(8, BLK, CHIPS, BLK)


def solution(mesh):
    in_specs = (
        P(None, "row", None, "col"),
        P("row", None, None),
        P("row", None, None),
        P(),
        P(),
        P(),
    )
    out_specs = P(None, "row", None, "col")
    return jax.shard_map(shards, mesh=mesh, in_specs=in_specs, out_specs=out_specs, check_vma=False)
```
